128 devices in a mesh: dp: 4 (over z_hi, core), ctx: 32 (over z_lo, y, x).
Axes of the slice: x: 4, y: 4, z: 4 (z_hi: 2, z_lo: 2; z = z_hi * 2 + z_lo), core: 2. Of those that a mesh axis runs over, the one named last changes fastest.
Arguments:
- density: float32 [512, 64, 64], P(('dp', 'ctx')), parts along dimension 0, may hold values from 0.1 to 50, as said below
- stem_weight: bfloat16 [216, 1024], replicated, may hold values from -0.4375 to 0.4375
- stem_bias: float32 [1024], replicated, may hold values from -3 to 3
- pos_embed: bfloat16 [8192, 1024], P('ctx'), may hold values from -3 to 3
- ln1_gain: float32 [1024], replicated, may hold values from 0.25 to 1.75
- ln1_bias: float32 [1024], replicated, may hold values from -2 to 2
- w_qkv: bfloat16 [1024, 3072], replicated, may hold values from -2 to 2
- qkv_bias: float32 [3072], replicated, may hold values from -2 to 2
- w_out: bfloat16 [1024, 1024], replicated, may hold values from -0.1875 to 0.1875
- out_bias: float32 [1024], replicated, may hold values from -2 to 2
- ln2_gain: float32 [1024], replicated, may hold values from 0.25 to 1.75
- ln2_bias: float32 [1024], replicated, may hold values from -2 to 2
- w_fc1: bfloat16 [1024, 4096], replicated, may hold values from -0.1875 to 0.1875
- fc1_bias: float32 [4096], replicated, may hold values from -3 to 3
- w_fc2: bfloat16 [4096, 1024], replicated, may hold values from -0.09375 to 0.09375
- fc2_bias: float32 [1024], replicated, may hold values from -2 to 2
Outputs:
- encoded: bfloat16 [32768, 1024], P(('dp', 'ctx')), parts along dimension 0
The draws below stay inside these ranges and needn't reach their ends.
There are 4 independent parts, one for each index of `dp`. The reference program is written for one: setup_inputs(seed, part) draws one part's arguments, and reference() takes and returns one part's arrays. A program takes and returns all parts, laid end to end along the dimension named above; an argument that names none is the same for every part. Nothing has to cross between parts.
Inputs may be any that keep to these rules, and one draw needn't show every extreme that they name: density is positive.
All inputs are finite; a program needn't handle non-finite values.
Results may differ from the reference program's by a relative error of at most 0.013.
Values may be sent and summed in bfloat16 or wider, within the bound.
A program may use at most 384 MiB of HBM per device.

```python
import math
import jax
import jax.numpy as jnp
from jax import lax

D = 1024
FF = 4096
HEADS = 16
KERNEL = 6
STRIDE = 4
GYZ = 16
TX = 32
TOKENS = 8192


def draw_density(key, part):
    planes = STRIDE * TX
    side_cells = STRIDE * GYZ
    key_one = jax.random.fold_in(key, 11)
    gradient = jnp.arange(planes, dtype=jnp.float32)[:, None, None] / max(planes - 1, 1)
    entries = jnp.exp(jax.random.uniform(key_one, (planes, side_cells, side_cells), jnp.float32, math.log(0.2), math.log(5.0)))
    scaling = jnp.exp(math.log(3.0) * gradient)
    return entries * scaling


def draw_w_qkv(key, part):
    key_one = jax.random.fold_in(jax.random.fold_in(key, 23), 0)
    spread = 1.6 / math.sqrt(D)
    return (jnp.clip(jax.random.normal(key_one, (D, 3 * D), jnp.float32), -6.0, 6.0) * spread).astype(jnp.bfloat16)


def block_scale(stream_key, extent, shards, low, top_value):
    def one(position, parts):
        draws = jax.random.uniform(jax.random.fold_in(jax.random.fold_in(stream_key, 6), position), (parts,), jnp.float32, low / len(shards), top_value / len(shards))
        return jnp.repeat(jnp.exp(draws), extent[position] // parts).reshape((-1,) + (1,) * (len(extent) - position - 1))

    level = one(*shards[0])
    for cut in shards[1:]:
        level = level * one(*cut)
    return level


def scatter_about(key, extent, scale, most, cuts=(), kind=jnp.bfloat16):
    gain = block_scale(key, extent, cuts, -0.22, 0.18) if cuts else 1.0
    values = jax.random.normal(key, extent, jnp.float32) * scale * gain
    return jnp.minimum(jnp.maximum(values, -most), most).astype(kind)


def setup_inputs(seed: int = 0, part: int = 0) -> dict:
    key_list = jax.random.split(jax.random.key(seed), 17)
    part_keys = jax.random.split(jax.random.fold_in(key_list[16], part), 17)
    return {
        "density": draw_density(jax.random.fold_in(jax.random.fold_in(key_list[16], part), 71), part),
        "stem_weight": scatter_about(key_list[1], (KERNEL * KERNEL * KERNEL, D), (KERNEL * KERNEL * KERNEL) ** -0.5, 0.4375),
        "stem_bias": scatter_about(key_list[2], (D,), 0.5, 3.0, (), jnp.float32),
        "pos_embed": scatter_about(key_list[3], (TOKENS, D), 0.5, 3.0, ((0, 32),)),
        "ln1_gain": jnp.clip(1.0 + 0.15 * jax.random.normal(key_list[4], (D,), jnp.float32), 0.25, 1.75),
        "ln1_bias": scatter_about(key_list[5], (D,), 0.3, 2.0, (), jnp.float32),
        "w_qkv": draw_w_qkv(jax.random.fold_in(key_list[16], 71), part),
        "qkv_bias": scatter_about(key_list[7], (3 * D,), 0.3, 2.0, (), jnp.float32),
        "w_out": scatter_about(key_list[8], (D, D), D ** -0.5, 0.1875),
        "out_bias": scatter_about(key_list[9], (D,), 0.3, 2.0, (), jnp.float32),
        "ln2_gain": jnp.clip(1.0 + 0.15 * jax.random.normal(key_list[10], (D,), jnp.float32), 0.25, 1.75),
        "ln2_bias": scatter_about(key_list[11], (D,), 0.3, 2.0, (), jnp.float32),
        "w_fc1": scatter_about(key_list[12], (D, FF), D ** -0.5, 0.1875),
        "fc1_bias": scatter_about(key_list[13], (FF,), 0.5, 3.0, (), jnp.float32),
        "w_fc2": scatter_about(key_list[14], (FF, D), FF ** -0.5, 0.09375),
        "fc2_bias": scatter_about(key_list[15], (D,), 0.3, 2.0, (), jnp.float32),
    }


def layer_norm(inputs, gain_vector, shift_vector):
    values = inputs.astype(jnp.float32)
    center = values - lax.optimization_barrier(jnp.mean(values, axis=-1, keepdims=True))
    spread = lax.optimization_barrier(jnp.mean(center * center, axis=-1, keepdims=True))
    return center * lax.rsqrt(spread + 1e-06) * gain_vector + shift_vector

def stem_conv(stacked, stem_weight):
    model_width = stem_weight.shape[1]
    kernel = stem_weight.reshape(6, 6, 6, 1, model_width)
    result = lax.conv_general_dilated(stacked[..., None], kernel, (4, 4, 4), ((1, 1), (1, 1), (1, 1)), dimension_numbers=('NDHWC', 'DHWIO', 'NDHWC'), preferred_element_type=jnp.float32)
    return result.reshape(-1, model_width)

def single_head(triple):
    query_head, key_head, value_head = triple
    scores = jnp.dot(query_head, key_head.T, preferred_element_type=jnp.float32)
    row_max = lax.optimization_barrier(jnp.max(scores, axis=1, keepdims=True))
    weights = jnp.exp(scores - row_max)
    row_total = lax.optimization_barrier(jnp.sum(weights, axis=1, keepdims=True))
    mixed = jnp.dot(weights.astype(jnp.bfloat16), value_head, preferred_element_type=jnp.float32) / row_total
    return mixed.astype(jnp.bfloat16)

def reference(density, stem_weight, stem_bias, pos_embed, ln1_gain, ln1_bias, w_qkv, qkv_bias, w_out, out_bias, ln2_gain, ln2_bias, w_fc1, fc1_bias, w_fc2, fc2_bias):
    model_width = w_out.shape[0]
    head_size = model_width // HEADS
    mean_density = jnp.mean(density)
    field = jnp.log(density / mean_density).astype(jnp.bfloat16)
    embedded = stem_conv(field[None], stem_weight) + stem_bias + pos_embed.astype(jnp.float32)
    residual = embedded.astype(jnp.bfloat16)
    normed = layer_norm(residual, ln1_gain, ln1_bias).astype(jnp.bfloat16)
    projected = jnp.dot(normed, w_qkv, preferred_element_type=jnp.float32) + qkv_bias
    token_count = normed.shape[0]
    query_rows = (projected[:, :model_width] * (1.0 / head_size ** 0.5)).astype(jnp.bfloat16)
    key_rows = projected[:, model_width:2 * model_width].astype(jnp.bfloat16)
    value_rows = projected[:, 2 * model_width:].astype(jnp.bfloat16)

    def split_heads(matrix):
        return matrix.reshape(token_count, HEADS, head_size).transpose(1, 0, 2)
    attended = lax.map(single_head, (split_heads(query_rows), split_heads(key_rows), split_heads(value_rows)))
    attended = attended.transpose(1, 0, 2).reshape(token_count, model_width)
    stream = (residual.astype(jnp.float32) + jnp.dot(attended, w_out, preferred_element_type=jnp.float32) + out_bias).astype(jnp.bfloat16)
    normed_two = layer_norm(stream, ln2_gain, ln2_bias).astype(jnp.bfloat16)
    hidden = jax.nn.gelu(jnp.dot(normed_two, w_fc1, preferred_element_type=jnp.float32) + fc1_bias, approximate=False).astype(jnp.bfloat16)
    encoded = stream.astype(jnp.float32) + jnp.dot(hidden, w_fc2, preferred_element_type=jnp.float32) + fc2_bias
    return encoded.astype(jnp.bfloat16)
```

```python
import math

import jax
import jax.numpy as jnp
from jax import lax
from jax.experimental import pallas as pl
from jax.experimental.pallas import tpu as pltpu
from jax.sharding import PartitionSpec as P

F32 = jnp.float32
BF16 = jnp.bfloat16
HEADS = 16
HEAD = 64
VROWS = 80
PLANE = 16


def from_everyone(value, axis):
    copies = jnp.broadcast_to(value, (lax.axis_size(axis), *value.shape))
    return lax.all_to_all(copies, axis, split_axis=0, concat_axis=0, tiled=True)


def over_copies(value, axis):
    return from_everyone(value, axis).sum(axis=0)


def padded_2(block, axis, dim, width):
    count = lax.axis_size(axis)
    forward = [(i, i + 1) for i in range(count - 1)]
    backward = [(target, source) for source, target in forward]
    low = lax.ppermute(lax.slice_in_dim(block, block.shape[dim] - width, None, axis=dim), axis, forward)
    high = lax.ppermute(lax.slice_in_dim(block, 0, width, axis=dim), axis, backward)
    return jnp.concatenate([low, block, high], axis=dim)


def layer_norm(inputs, gain_vector, shift_vector):
    values = inputs.astype(F32)
    center = values - jnp.mean(values, axis=-1, keepdims=True)
    spread = jnp.mean(center * center, axis=-1, keepdims=True)
    return center * lax.rsqrt(spread + 1e-06) * gain_vector + shift_vector


def slab_conv(stacked, stem_weight):
    model_width = stem_weight.shape[1]
    kernel = stem_weight.reshape(6, 6, 6, 1, model_width)
    result = lax.conv_general_dilated(
        stacked[..., None],
        kernel,
        (4, 4, 4),
        ((0, 0), (1, 1), (1, 1)),
        dimension_numbers=("NDHWC", "DHWIO", "NDHWC"),
        preferred_element_type=F32,
    )
    return result.reshape(stacked.shape[0], -1, model_width)


def attention(query, mine, other):
    parts, _, tokens = query.shape
    keys = 2 * parts * tokens
    group = 4
    width = group * tokens
    chunk = 512
    steps = keys // chunk

    def kernel(q_ref, a_ref, b_ref, o_ref, k_s, v_s, s_s):
        @pl.when(pl.program_id(0) == 0)
        def _():
            for part, ref in enumerate((a_ref, b_ref)):
                for i in range(parts):
                    at = (part * parts + i) * tokens
                    k_s[at : at + tokens, :] = ref[i, 0:HEAD, :].T
                    v_s[0:HEAD, at : at + tokens] = ref[i, HEAD : 2 * HEAD, :]
            row = lax.broadcasted_iota(jnp.int32, (VROWS - HEAD, keys), 0)
            v_s[HEAD:VROWS, :] = jnp.where(row == 0, 1.0, 0.0).astype(BF16)

        q = jnp.concatenate([q_ref[i] for i in range(group)], axis=1)

        def scores(c):
            at = pl.multiple_of(c * chunk, chunk)
            return jnp.dot(k_s[pl.ds(at, chunk), :], q, preferred_element_type=F32)

        first = scores(0)
        s_s[0] = first
        top = jnp.max(first, axis=0, keepdims=True)

        def body(i, carry):
            high, total, top = carry
            for slot in range(2):
                c = 2 * i + slot
                raised = jnp.maximum(high, top)
                fade = jnp.exp2(high - raised)
                weights = jnp.exp2(s_s[slot] - raised).astype(BF16)
                at = pl.multiple_of(c * chunk, chunk)
                ahead = scores(jnp.minimum(c + 1, steps - 1))
                s_s[1 - slot] = ahead
                top = jnp.max(ahead, axis=0, keepdims=True)
                total = total * fade + jnp.dot(
                    v_s[:, pl.ds(at, chunk)], weights, preferred_element_type=F32
                )
                high = raised
            return high, total, top

        _, total, _ = lax.fori_loop(
            0,
            steps // 2,
            body,
            (jnp.full((1, width), -1e30, F32), jnp.zeros((VROWS, width), F32), top),
        )
        mixed = (total[0:HEAD] / total[HEAD : HEAD + 1]).astype(BF16)
        for i in range(group):
            o_ref[i] = mixed[:, i * tokens : (i + 1) * tokens]

    whole = pl.BlockSpec((parts, 2 * HEAD, tokens), lambda i: (0, 0, 0))
    block = pl.BlockSpec((group, HEAD, tokens), lambda i: (i, 0, 0))
    return pl.pallas_call(
        kernel,
        grid=(parts // group,),
        in_specs=[block, whole, whole],
        out_specs=block,
        out_shape=jax.ShapeDtypeStruct(query.shape, BF16),
        scratch_shapes=[
            pltpu.VMEM((keys, HEAD), BF16),
            pltpu.VMEM((VROWS, keys), BF16),
            pltpu.VMEM((2, chunk, width), F32),
        ],
        compiler_params=pltpu.CompilerParams(vmem_limit_bytes=56 * 2**20),
        name="attention",
    )(query, mine, other)


def per_device(
    density, stem_weight, stem_bias, pos_embed, ln1_gain, ln1_bias, w_qkv, qkv_bias,
    w_out, out_bias, ln2_gain, ln2_bias, w_fc1, fc1_bias, w_fc2, fc2_bias,
):
    model_width = w_out.shape[0]
    cell_count = density.size * lax.axis_size("ctx")
    mean_density = over_copies(jnp.sum(density), "ctx") / cell_count
    source = jnp.log(density / mean_density).astype(BF16)
    padded = padded_2(source, "ctx", 0, 1)
    embedded = slab_conv(padded[None], stem_weight)[0]
    embedded = embedded + stem_bias + pos_embed.astype(F32)
    residual = embedded.astype(BF16)
    normed = layer_norm(residual, ln1_gain, ln1_bias).astype(BF16)
    tokens = normed.shape[0]
    projected = jnp.einsum("tk,kf->ft", normed, w_qkv, preferred_element_type=F32) + qkv_bias[:, None]
    scale = math.log2(math.e) / math.sqrt(HEAD)
    q = (projected[:model_width] * scale).astype(BF16).reshape(HEADS, HEAD, tokens)
    k = projected[model_width : 2 * model_width].astype(BF16).reshape(HEADS, HEAD, tokens)
    v = projected[2 * model_width :].astype(BF16).reshape(HEADS, HEAD, tokens)
    planes = [list(range(PLANE)), list(range(PLANE, 2 * PLANE))]
    swap = [(i, (i + PLANE) % (2 * PLANE)) for i in range(2 * PLANE)]
    kv = lax.all_to_all(
        jnp.concatenate([k, v], axis=1), "ctx", 0, 0, axis_index_groups=planes, tiled=True
    )
    other = lax.ppermute(kv, "ctx", swap)
    q = lax.all_to_all(q, "ctx", 0, 0, axis_index_groups=planes, tiled=True)
    mixed = attention(q, kv, other)
    back = lax.all_to_all(mixed, "ctx", 0, 0, axis_index_groups=planes, tiled=True)
    attended = back.reshape(model_width, tokens)
    stream = (
        residual.astype(F32)
        + jnp.einsum("ft,fd->td", attended, w_out, preferred_element_type=F32)
        + out_bias
    ).astype(BF16)
    normed_two = layer_norm(stream, ln2_gain, ln2_bias).astype(BF16)
    hidden = jax.nn.gelu(
        jnp.dot(normed_two, w_fc1, preferred_element_type=F32) + fc1_bias, approximate=False
    ).astype(BF16)
    encoded = (
        stream.astype(F32) + jnp.dot(hidden, w_fc2, preferred_element_type=F32) + fc2_bias
    )
    return encoded.astype(BF16)


def solution(mesh):
    in_specs = (P(("dp", "ctx"), None, None), P(), P(), P("ctx", None)) + (P(),) * 12
    return jax.shard_map(
        per_device, mesh=mesh, in_specs=in_specs, out_specs=P(("dp", "ctx"), None), check_vma=False
    )
```

```python
import math

import jax
import jax.numpy as jnp
from jax import lax
from jax.experimental import pallas as pl
from jax.experimental.pallas import tpu as pltpu
from jax.sharding import PartitionSpec as P

F32 = jnp.float32
BF16 = jnp.bfloat16
HEADS = 16
HEAD = 64
VROWS = 80
PLANE = 16
ROW = 4
MESH = pl.DeviceIdType.MESH
VMEM_LIMIT = 58 * 2**20


def remote(src, dst, send, recv, index):
    return pltpu.make_async_remote_copy(
        src_ref=src,
        dst_ref=dst,
        send_sem=send,
        recv_sem=recv,
        device_id={"ctx": index},
        device_id_type=MESH,
    )


def greet(peers):
    barrier = pltpu.get_barrier_semaphore()
    for peer in peers:
        pl.semaphore_signal(barrier, inc=1, device_id={"ctx": peer}, device_id_type=MESH)
    return barrier


def normalize(rows, gain, shift):
    center = rows - jnp.mean(rows, axis=-1, keepdims=True)
    spread = jnp.mean(center * center, axis=-1, keepdims=True)
    return center * lax.rsqrt(spread + 1e-06) * gain + shift


def plane_order(me):
    y, x = lax.rem(lax.div(me, ROW), ROW), lax.rem(me, ROW)
    order = []
    for i in (0, 1, 3, 2):
        for j in range(ROW):
            order.append((i, j, lax.rem(y + i, ROW), lax.rem(x + j, ROW)))
    return order


def front(density, stem_weight, stem_bias, pos, gain, shift, w_qkv, qkv_bias, cells):
    planes, side, _ = density.shape
    count = lax.axis_size("ctx")
    width = stem_weight.shape[1]
    tokens = pos.shape[0]
    grid = side // 4
    lanes = grid * 128
    scale = math.log2(math.e) / math.sqrt(HEAD)
    pad = 72

    def kernel(
        d_ref, ws_ref, sb_ref, pos_ref, g_ref, b_ref, wq_ref, qb_ref,
        res_ref, q_ref, kv_ref,
        mine, sums, halo, fp, x6, w6, wq, posv, blocks,
        sum_s, sum_r, halo_s, halo_r, q_s, q_r, kv_s, kv_r, f_s, f_r, load,
    ):
        me = lax.axis_index("ctx")
        half = lax.div(me, PLANE)
        here = lax.rem(me, PLANE)
        peers = [lax.rem(me + i, count) for i in range(1, count)]
        barrier = greet(peers)
        load_w = pltpu.make_async_copy(wq_ref, wq, load.at[0])
        load_w.start()
        load_p = pltpu.make_async_copy(pos_ref, posv, load.at[1])
        load_p.start()

        slab = d_ref[...]
        part = jnp.sum(slab, axis=0)
        part = jnp.sum(part, axis=0, keepdims=True)
        part = jnp.sum(part, axis=1, keepdims=True)
        mine[...] = jnp.broadcast_to(part, (8, 128))
        pl.semaphore_wait(barrier, count - 1)

        up, down = peers[0], peers[-1]
        to_up = remote(d_ref.at[planes - 1], halo.at[0], halo_s.at[0], halo_r.at[0], up)
        to_down = remote(d_ref.at[0], halo.at[1], halo_s.at[1], halo_r.at[1], down)
        to_up.start()
        to_down.start()
        shares = []
        for i, peer in enumerate(peers):
            shares.append(remote(mine, sums.at[i], sum_s.at[i], sum_r.at[i], peer))
            shares[-1].start()

        fp[...] = jnp.zeros(fp.shape, F32)
        w6[...] = jnp.zeros(w6.shape, BF16)
        for a in range(6):
            w6[a * 128 : a * 128 + 36, :] = ws_ref[a * 36 : (a + 1) * 36, :]

        for share in shares:
            share.wait()
        to_up.wait()
        to_down.wait()
        total = mine[...] + jnp.sum(sums[...], axis=0)
        mean = (total / cells)[0:1, 0:1]

        def logged(values):
            return jnp.log(values / mean).astype(BF16).astype(F32)

        low = jnp.where(me > 0, logged(halo[0]), 0.0)
        high = jnp.where(me < count - 1, logged(halo[1]), 0.0)
        own = logged(slab.reshape(planes * side, side))
        fp[1 : 1 + side, 0:side] = low
        for a in range(planes):
            at = (a + 1) * pad + 1
            fp[at : at + side, 0:side] = own[a * side : (a + 1) * side, :]
        at = (planes + 1) * pad + 1
        fp[at : at + side, 0:side] = high

        z = lax.broadcasted_iota(jnp.int32, (side, lanes), 0)
        col = lax.broadcasted_iota(jnp.int32, (side, lanes), 1)
        lane = jnp.bitwise_and(col, 127)
        base = z + 1 - 4 * jnp.right_shift(col, 7) - lane
        spread = jnp.zeros((6 * grid, lanes), F32)
        for b in range(6):
            rows = jnp.concatenate(
                [fp[pl.ds(a * pad + b, grid, stride=4), 0:side] for a in range(6)], axis=0
            )
            pick = (base == -6 * b) & (lane >= 6 * b) & (lane < 6 * b + 6)
            spread += jnp.dot(
                rows.astype(BF16),
                jnp.where(pick, 1.0, 0.0).astype(BF16),
                preferred_element_type=F32,
            )
        spread = spread.astype(BF16)
        for k in range(grid):
            for a in range(6):
                x6[k * grid : (k + 1) * grid, a * 128 : (a + 1) * 128] = spread[
                    a * grid : (a + 1) * grid, k * 128 : (k + 1) * 128
                ]
        r = lax.broadcasted_iota(jnp.int32, (tokens, tokens), 0)
        s = lax.broadcasted_iota(jnp.int32, (tokens, tokens), 1)
        turn = (jnp.right_shift(r, 4) == jnp.bitwise_and(s, 15)) & (
            jnp.bitwise_and(r, 15) == jnp.right_shift(s, 4)
        )
        patches = jnp.dot(
            jnp.where(turn, 1.0, 0.0).astype(BF16), x6[...], preferred_element_type=F32
        ).astype(BF16)
        load_p.wait()
        embedded = (
            jnp.dot(patches, w6[...], preferred_element_type=F32)
            + sb_ref[...]
            + posv[...].astype(F32)
        )
        residual = embedded.astype(BF16)
        res_ref[...] = residual
        normed = normalize(residual.astype(F32), g_ref[...], b_ref[...]).astype(BF16)

        load_w.wait()
        order = plane_order(me)
        sends = []
        for n, (i, j, row, column) in enumerate(order):
            if j == 0:
                for part_index in range(3):
                    at = pl.multiple_of(part_index * width + row * 256, 256)
                    out = (
                        jnp.dot(normed, wq[:, pl.ds(at, 256)], preferred_element_type=F32)
                        + qb_ref[:, pl.ds(at, 256)]
                    )
                    if part_index == 0:
                        out = out * scale
                    turned = out.T.astype(BF16)
                    for k in range(ROW):
                        blocks[
                            row * ROW + k, part_index * HEAD : (part_index + 1) * HEAD, :
                        ] = turned[k * HEAD : (k + 1) * HEAD, :]
            head = row * ROW + column
            q_src = blocks.at[head, 0:HEAD]
            kv_src = blocks.at[head, HEAD : 3 * HEAD]
            if n == 0:
                own_q = pltpu.make_async_copy(q_src, q_ref.at[here], load.at[2])
                own_kv = pltpu.make_async_copy(kv_src, kv_ref.at[0, here], load.at[3])
                own_q.start()
                own_kv.start()
            else:
                to = half * PLANE + head
                kv_copy = remote(kv_src, kv_ref.at[0, here], kv_s.at[n], kv_r.at[n], to)
                q_copy = remote(q_src, q_ref.at[here], q_s.at[n], q_r.at[n], to)
                kv_copy.start()
                q_copy.start()
                sends.append((kv_copy, q_copy))

        y, x = lax.rem(lax.div(me, ROW), ROW), lax.rem(me, ROW)
        beside = (1 - half) * PLANE + here
        forwards = []
        for n, (i, j, _, _) in enumerate(order):
            source = lax.rem(y + ROW - i, ROW) * ROW + lax.rem(x + ROW - j, ROW)
            if n == 0:
                passed = remote(
                    blocks.at[here, HEAD : 3 * HEAD], kv_ref.at[1, here], f_s.at[n], f_r.at[n], beside
                )
            else:
                remote(
                    blocks.at[here, HEAD : 3 * HEAD],
                    kv_ref.at[0, source],
                    kv_s.at[n],
                    kv_r.at[n],
                    me,
                ).wait_recv()
                passed = remote(
                    kv_ref.at[0, source], kv_ref.at[1, source], f_s.at[n], f_r.at[n], beside
                )
            passed.start()
            forwards.append(passed)
        own_q.wait()
        own_kv.wait()
        for kv_copy, q_copy in sends:
            q_copy.wait()
            kv_copy.wait_send()
        for passed in forwards:
            passed.wait()

    vmem = pl.BlockSpec(memory_space=pltpu.VMEM)
    anywhere = pl.BlockSpec(memory_space=pl.ANY)
    dma = pltpu.SemaphoreType.DMA
    return pl.pallas_call(
        kernel,
        in_specs=[vmem, vmem, vmem, anywhere, vmem, vmem, anywhere, vmem],
        out_specs=[vmem, anywhere, anywhere],
        out_shape=[
            jax.ShapeDtypeStruct((tokens, width), BF16),
            jax.ShapeDtypeStruct((PLANE, HEAD, tokens), BF16),
            jax.ShapeDtypeStruct((2, PLANE, 2 * HEAD, tokens), BF16),
        ],
        scratch_shapes=[
            pltpu.VMEM((8, 128), F32),
            pltpu.VMEM((count - 1, 8, 128), F32),
            pltpu.VMEM((2, side, side), F32),
            pltpu.VMEM((6 * pad, 128), F32),
            pltpu.VMEM((tokens, 6 * 128), BF16),
            pltpu.VMEM((6 * 128, width), BF16),
            pltpu.VMEM(w_qkv.shape, BF16),
            pltpu.VMEM(pos.shape, BF16),
            pltpu.VMEM((HEADS, 3 * HEAD, tokens), BF16),
            dma((count - 1,)), dma((count - 1,)), dma((2,)), dma((2,)),
            dma((PLANE,)), dma((PLANE,)), dma((PLANE,)), dma((PLANE,)),
            dma((PLANE,)), dma((PLANE,)), dma((4,)),
        ],
        compiler_params=pltpu.CompilerParams(
            vmem_limit_bytes=VMEM_LIMIT, collective_id=0, has_side_effects=True
        ),
        name="front",
    )(density, stem_weight, stem_bias, pos, gain, shift, w_qkv, qkv_bias)


def attention(query, keys_values):
    parts, _, tokens = query.shape
    sources = keys_values.shape[0]
    keys = sources * tokens
    group = 4
    width = group * tokens
    chunk = 512
    steps = keys // chunk

    def kernel(q_ref, kv_ref, o_ref, k_s, v_s, s_s):
        @pl.when(pl.program_id(0) == 0)
        def _():
            for i in range(sources):
                at = i * tokens
                k_s[at : at + tokens, :] = kv_ref[i, 0:HEAD, :].T
                v_s[0:HEAD, at : at + tokens] = kv_ref[i, HEAD : 2 * HEAD, :]
            row = lax.broadcasted_iota(jnp.int32, (VROWS - HEAD, keys), 0)
            v_s[HEAD:VROWS, :] = jnp.where(row == 0, 1.0, 0.0).astype(BF16)

        q = jnp.concatenate([q_ref[i] for i in range(group)], axis=1)

        def scores(c):
            at = pl.multiple_of(c * chunk, chunk)
            return jnp.dot(k_s[pl.ds(at, chunk), :], q, preferred_element_type=F32)

        first = scores(0)
        s_s[0] = first
        top = jnp.max(first, axis=0, keepdims=True)

        def body(i, carry):
            high, total, top = carry
            for slot in range(2):
                c = 2 * i + slot
                raised = jnp.maximum(high, top)
                fade = jnp.exp2(high - raised)
                weights = jnp.exp2(s_s[slot] - raised).astype(BF16)
                at = pl.multiple_of(c * chunk, chunk)
                ahead = scores(jnp.minimum(c + 1, steps - 1))
                s_s[1 - slot] = ahead
                top = jnp.max(ahead, axis=0, keepdims=True)
                total = total * fade + jnp.dot(
                    v_s[:, pl.ds(at, chunk)], weights, preferred_element_type=F32
                )
                high = raised
            return high, total, top

        _, total, _ = lax.fori_loop(
            0,
            steps // 2,
            body,
            (jnp.full((1, width), -1e30, F32), jnp.zeros((VROWS, width), F32), top),
        )
        mixed = (total[0:HEAD] / total[HEAD : HEAD + 1]).astype(BF16)
        for i in range(group):
            o_ref[i] = mixed[:, i * tokens : (i + 1) * tokens]

    whole = pl.BlockSpec(keys_values.shape, lambda i: (0, 0, 0))
    block = pl.BlockSpec((group, HEAD, tokens), lambda i: (i, 0, 0))
    return pl.pallas_call(
        kernel,
        grid=(parts // group,),
        in_specs=[block, whole],
        out_specs=block,
        out_shape=jax.ShapeDtypeStruct(query.shape, BF16),
        scratch_shapes=[
            pltpu.VMEM((keys, HEAD), BF16),
            pltpu.VMEM((VROWS, keys), BF16),
            pltpu.VMEM((2, chunk, width), F32),
        ],
        compiler_params=pltpu.CompilerParams(vmem_limit_bytes=VMEM_LIMIT),
        name="attention",
    )(query, keys_values)


def tail(mixed, residual, w_out, out_bias, gain, shift, w1, b1, w2, b2):
    tokens, width = residual.shape
    hidden_width = w1.shape[1]
    step = 512

    def kernel(
        o_ref, res_ref, wo_ref, ob_ref, g_ref, b_ref, w1_ref, b1_ref, w2_ref, b2_ref,
        out_ref,
        att, wo, w1v, w2v, send, recv, load,
    ):
        me = lax.axis_index("ctx")
        half = lax.div(me, PLANE)
        here = lax.rem(me, PLANE)
        order = plane_order(me)
        targets = [half * PLANE + row * ROW + column for _, _, row, column in order]
        barrier = greet(targets[1:])
        loads = [
            pltpu.make_async_copy(wo_ref, wo, load.at[0]),
            pltpu.make_async_copy(w1_ref, w1v, load.at[1]),
            pltpu.make_async_copy(w2_ref, w2v, load.at[2]),
        ]
        for copy in loads:
            copy.start()
        own = pltpu.make_async_copy(o_ref.at[here], att.at[here], load.at[3])
        own.start()
        pl.semaphore_wait(barrier, PLANE - 1)
        sends = []
        for n, (_, _, row, column) in enumerate(order):
            if n:
                copy = remote(
                    o_ref.at[row * ROW + column], att.at[here], send.at[n], recv.at[n], targets[n]
                )
                copy.start()
                sends.append(copy)
        own.wait()
        for copy in sends:
            copy.wait()
        loads[0].wait()
        attended = att[...].reshape(width, tokens).T
        stream = (
            res_ref[...].astype(F32)
            + jnp.dot(attended, wo[...], preferred_element_type=F32)
            + ob_ref[...]
        ).astype(BF16)
        rows = stream.astype(F32)
        normed = normalize(rows, g_ref[...], b_ref[...]).astype(BF16)
        loads[1].wait()
        loads[2].wait()

        def body(c, total):
            at = pl.multiple_of(c * step, step)
            hidden = (
                jnp.dot(normed, w1v[:, pl.ds(at, step)], preferred_element_type=F32)
                + b1_ref[:, pl.ds(at, step)]
            )
            hidden = 0.5 * hidden * (1.0 + lax.erf(hidden * math.sqrt(0.5)))
            return total + jnp.dot(
                hidden.astype(BF16), w2v[pl.ds(at, step), :], preferred_element_type=F32
            )

        total = lax.fori_loop(0, hidden_width // step, body, rows + b2_ref[...])
        out_ref[...] = total.astype(BF16)

    vmem = pl.BlockSpec(memory_space=pltpu.VMEM)
    anywhere = pl.BlockSpec(memory_space=pl.ANY)
    dma = pltpu.SemaphoreType.DMA
    return pl.pallas_call(
        kernel,
        in_specs=[vmem, vmem, anywhere, vmem, vmem, vmem, anywhere, vmem, anywhere, vmem],
        out_specs=vmem,
        out_shape=jax.ShapeDtypeStruct((tokens, width), BF16),
        scratch_shapes=[
            pltpu.VMEM(mixed.shape, BF16),
            pltpu.VMEM(w_out.shape, BF16),
            pltpu.VMEM(w1.shape, BF16),
            pltpu.VMEM(w2.shape, BF16),
            dma((PLANE,)), dma((PLANE,)), dma((4,)),
        ],
        compiler_params=pltpu.CompilerParams(
            vmem_limit_bytes=VMEM_LIMIT, collective_id=1, has_side_effects=True
        ),
        name="tail",
    )(mixed, residual, w_out, out_bias, gain, shift, w1, b1, w2, b2)


def per_device(
    density, stem_weight, stem_bias, pos_embed, ln1_gain, ln1_bias, w_qkv, qkv_bias,
    w_out, out_bias, ln2_gain, ln2_bias, w_fc1, fc1_bias, w_fc2, fc2_bias,
):
    def flat(vector):
        return vector.reshape(1, -1)

    cells = float(density.size * lax.axis_size("ctx"))
    residual, query, keys_values = front(
        density, stem_weight, flat(stem_bias), pos_embed, flat(ln1_gain), flat(ln1_bias),
        w_qkv, flat(qkv_bias), cells,
    )
    mixed = attention(query, keys_values.reshape(2 * PLANE, 2 * HEAD, -1))
    return tail(
        mixed, residual, w_out, flat(out_bias), flat(ln2_gain), flat(ln2_bias),
        w_fc1, flat(fc1_bias), w_fc2, flat(fc2_bias),
    )


def solution(mesh):
    in_specs = (P(("dp", "ctx"), None, None), P(), P(), P("ctx", None)) + (P(),) * 12
    return jax.shard_map(
        per_device, mesh=mesh, in_specs=in_specs, out_specs=P(("dp", "ctx"), None), check_vma=False
    )
```

```python
import math

import jax
import jax.numpy as jnp
from jax import lax
from jax.experimental import pallas as pl
from jax.experimental.pallas import tpu as pltpu
from jax.sharding import PartitionSpec as P

F32 = jnp.float32
BF16 = jnp.bfloat16
HEADS = 16
HEAD = 64
VROWS = 80
PLANE = 16
ROW = 4
MESH = pl.DeviceIdType.MESH
VMEM_LIMIT = 58 * 2**20


def remote(src, dst, send, recv, index):
    return pltpu.make_async_remote_copy(
        src_ref=src,
        dst_ref=dst,
        send_sem=send,
        recv_sem=recv,
        device_id={"ctx": index},
        device_id_type=MESH,
    )


def greet(peers):
    barrier = pltpu.get_barrier_semaphore()
    for peer in peers:
        pl.semaphore_signal(barrier, inc=1, device_id={"ctx": peer}, device_id_type=MESH)
    return barrier


def normalize(rows, gain, shift):
    center = rows - jnp.mean(rows, axis=-1, keepdims=True)
    spread = jnp.mean(center * center, axis=-1, keepdims=True)
    return center * lax.rsqrt(spread + 1e-06) * gain + shift


def plane_order(me):
    y, x = lax.rem(lax.div(me, ROW), ROW), lax.rem(me, ROW)
    order = []
    for i in (0, 1, 3, 2):
        for j in range(ROW):
            order.append((i, j, lax.rem(y + i, ROW), lax.rem(x + j, ROW)))
    return order


def encoder(
    density, stem_weight, stem_bias, pos, gain1, shift1, w_qkv, qkv_bias,
    w_out, out_bias, gain2, shift2, w1, b1, w2, b2, cells,
):
    planes, side, _ = density.shape
    count = lax.axis_size("ctx")
    width = stem_weight.shape[1]
    hidden_width = w1.shape[1]
    tokens = pos.shape[0]
    grid = side // 4
    lanes = grid * 128
    scale = math.log2(math.e) / math.sqrt(HEAD)
    pad = 72
    stages = 2 * ROW
    queries = ROW * tokens
    chunk = 2 * tokens
    step = 512

    def kernel(
        d_ref, ws_ref, sb_ref, pos_ref, g1_ref, s1_ref, wq_ref, qb_ref,
        wo_ref, ob_ref, g2_ref, s2_ref, w1_ref, b1_ref, w2_ref, b2_ref,
        out_ref,
        mine, sums, halo, fp, x6, w6, wq, posv, wo, w1v, w2v, resv,
        q_out, kv_out, q_in, kv_in, score, high_s, total_s, o_out, att,
        sum_s, sum_r, halo_s, halo_r, q_s, q_r, kv_s, kv_r, f_s, f_r, o_s, o_r, load,
    ):
        me = lax.axis_index("ctx")
        half = lax.div(me, PLANE)
        here = lax.rem(me, PLANE)
        y, x = lax.div(here, ROW), lax.rem(here, ROW)
        beside = (1 - half) * PLANE + here
        peers = [lax.rem(me + i, count) for i in range(1, count)]
        barrier = greet(peers)
        load_w = pltpu.make_async_copy(wq_ref, wq, load.at[0])
        load_w.start()
        load_p = pltpu.make_async_copy(pos_ref, posv, load.at[1])
        load_p.start()

        slab = d_ref[...]
        part = jnp.sum(slab, axis=0)
        part = jnp.sum(part, axis=0, keepdims=True)
        part = jnp.sum(part, axis=1, keepdims=True)
        mine[...] = jnp.broadcast_to(part, (8, 128))
        fp[...] = jnp.zeros(fp.shape, F32)
        w6[...] = jnp.zeros(w6.shape, BF16)
        for a in range(6):
            w6[a * 128 : a * 128 + 36, :] = ws_ref[a * 36 : (a + 1) * 36, :]
        pl.semaphore_wait(barrier, count - 1)

        up, down = peers[0], peers[-1]
        to_up = remote(d_ref.at[planes - 1], halo.at[0], halo_s.at[0], halo_r.at[0], up)
        to_down = remote(d_ref.at[0], halo.at[1], halo_s.at[1], halo_r.at[1], down)
        to_up.start()
        to_down.start()
        shares = []
        for i, peer in enumerate(peers):
            shares.append(remote(mine, sums.at[i], sum_s.at[i], sum_r.at[i], peer))
            shares[-1].start()
        for i in range(PLANE):
            q_in[i, 0:HEAD, :] = jnp.zeros((HEAD, tokens), BF16)
            q_in[i, 2 * HEAD : 3 * HEAD, :] = jnp.zeros((HEAD, tokens), BF16)
        for share in shares:
            share.wait()
        to_up.wait()
        to_down.wait()
        total = mine[...] + jnp.sum(sums[...], axis=0)
        mean = (total / cells)[0:1, 0:1]

        def logged(values):
            return jnp.log(values / mean).astype(BF16).astype(F32)

        low = jnp.where(me > 0, logged(halo[0]), 0.0)
        high = jnp.where(me < count - 1, logged(halo[1]), 0.0)
        own = logged(slab.reshape(planes * side, side))
        fp[1 : 1 + side, 0:side] = low
        for a in range(planes):
            at = (a + 1) * pad + 1
            fp[at : at + side, 0:side] = own[a * side : (a + 1) * side, :]
        at = (planes + 1) * pad + 1
        fp[at : at + side, 0:side] = high

        z = lax.broadcasted_iota(jnp.int32, (side, lanes), 0)
        col = lax.broadcasted_iota(jnp.int32, (side, lanes), 1)
        lane = jnp.bitwise_and(col, 127)
        base = z + 1 - 4 * jnp.right_shift(col, 7) - lane
        spread = jnp.zeros((6 * grid, lanes), F32)
        for b in range(6):
            rows = jnp.concatenate(
                [fp[pl.ds(a * pad + b, grid, stride=4), 0:side] for a in range(6)], axis=0
            )
            pick = (base == -6 * b) & (lane >= 6 * b) & (lane < 6 * b + 6)
            spread += jnp.dot(
                rows.astype(BF16),
                jnp.where(pick, 1.0, 0.0).astype(BF16),
                preferred_element_type=F32,
            )
        spread = spread.astype(BF16)
        for k in range(grid):
            for a in range(6):
                x6[k * grid : (k + 1) * grid, a * 128 : (a + 1) * 128] = spread[
                    a * grid : (a + 1) * grid, k * 128 : (k + 1) * 128
                ]
        r = lax.broadcasted_iota(jnp.int32, (tokens, tokens), 0)
        s = lax.broadcasted_iota(jnp.int32, (tokens, tokens), 1)
        turn = (jnp.right_shift(r, 4) == jnp.bitwise_and(s, 15)) & (
            jnp.bitwise_and(r, 15) == jnp.right_shift(s, 4)
        )
        patches = jnp.dot(
            jnp.where(turn, 1.0, 0.0).astype(BF16), x6[...], preferred_element_type=F32
        ).astype(BF16)
        load_p.wait()
        embedded = (
            jnp.dot(patches, w6[...], preferred_element_type=F32)
            + sb_ref[...]
            + posv[...].astype(F32)
        )
        residual = embedded.astype(BF16)
        resv[...] = residual
        normed = normalize(residual.astype(F32), g1_ref[...], s1_ref[...]).astype(BF16)

        load_w.wait()
        loads = [
            pltpu.make_async_copy(wo_ref, wo, load.at[2]),
            pltpu.make_async_copy(w1_ref, w1v, load.at[3]),
            pltpu.make_async_copy(w2_ref, w2v, load.at[4]),
        ]
        left = lax.broadcasted_iota(jnp.int32, (128, 128), 1) < HEAD
        order = plane_order(me)

        def project(part_index, row):
            at = pl.multiple_of(part_index * width + row * 256, 256)
            return (
                jnp.dot(normed, wq[:, pl.ds(at, 256)], preferred_element_type=F32)
                + qb_ref[:, pl.ds(at, 256)]
            )

        def make_q(row):
            turned = (project(0, row) * scale).T.astype(BF16)
            for k in range(ROW):
                q_out[row * ROW + k] = turned[k * HEAD : (k + 1) * HEAD, :]

        def make_kv(row):
            keys = project(1, row)
            turned = project(2, row).T.astype(BF16)
            for k in range(ROW):
                pair = keys[:, (k // 2) * 128 : (k // 2 + 1) * 128]
                lo, hi = pair[0:128], pair[128:256]
                if k % 2 == 0:
                    packed = jnp.where(left, lo, pltpu.roll(hi, HEAD, 1))
                else:
                    packed = jnp.where(left, pltpu.roll(lo, HEAD, 1), hi)
                at = row * ROW + k
                kv_out[at, 0:128, :] = packed.astype(BF16)
                kv_out[at, 128 : 128 + HEAD, :] = turned[k * HEAD : (k + 1) * HEAD, 0:128]
                kv_out[at, 128 + HEAD : 256, :] = turned[k * HEAD : (k + 1) * HEAD, 128:256]

        def q_copy(n):
            head = order[n][2] * ROW + order[n][3]
            return remote(
                q_out.at[head], q_in.at[n, HEAD : 2 * HEAD], q_s.at[n], q_r.at[n], half * PLANE + head
            )

        def kv_copy(n):
            head = order[n][2] * ROW + order[n][3]
            return remote(kv_out.at[head], kv_in.at[n], kv_s.at[n], kv_r.at[n], half * PLANE + head)

        for g in range(ROW):
            row = order[g * ROW][2]
            make_q(row)
            for n in range(g * ROW, (g + 1) * ROW):
                if n:
                    q_copy(n).start()
            if g == 0:
                make_kv(row)
                for n in range(1, ROW):
                    kv_copy(n).start()
        q_in[0, HEAD : 2 * HEAD, :] = q_out[here]
        kv_in[0] = kv_out[here]
        for g in range(1, ROW):
            make_kv(order[g * ROW][2])
            for n in range(g * ROW, (g + 1) * ROW):
                kv_copy(n).start()
        for copy in loads:
            copy.start()

        def forward(n):
            return remote(kv_in.at[n], kv_in.at[PLANE + n], f_s.at[n], f_r.at[n], beside)

        def arrived(n):
            remote(kv_in.at[n], kv_in.at[n], kv_s.at[n], kv_r.at[n], beside).wait_recv()

        def asked(n):
            remote(
                q_in.at[n, HEAD : 2 * HEAD], q_in.at[n, HEAD : 2 * HEAD], q_s.at[n], q_r.at[n], beside
            ).wait_recv()

        remote(kv_out.at[here], kv_in.at[PLANE], f_s.at[0], f_r.at[0], beside).start()
        for n in range(1, ROW):
            asked(n)
            arrived(n)
            forward(n).start()

        ones = jnp.where(
            lax.broadcasted_iota(jnp.int32, (VROWS - HEAD, 128), 0) == 0, 1.0, 0.0
        ).astype(BF16)

        def scores(u, c):
            g = lax.rem(u, ROW)
            n = lax.div(u, ROW) * ROW + 2 * c
            keys = kv_in[pl.ds(n, 2), 0:128, :].reshape(256, 128)
            lo = jnp.concatenate([q_in[g * ROW + k, HEAD : 3 * HEAD, :] for k in range(ROW)], axis=1)
            hi = jnp.concatenate([q_in[g * ROW + k, 0 : 2 * HEAD, :] for k in range(ROW)], axis=1)
            return jnp.concatenate(
                [
                    jnp.dot(keys, lo, preferred_element_type=F32),
                    jnp.dot(keys, hi, preferred_element_type=F32),
                ],
                axis=0,
            )

        def values(u, c):
            n = lax.div(u, ROW) * ROW + 2 * c
            pieces = []
            for at in (128, 128 + HEAD):
                for k in range(2):
                    pieces.append(
                        jnp.concatenate([kv_in[n + k, at : at + HEAD, :], ones], axis=0)
                    )
            return jnp.concatenate(pieces, axis=1)

        for g in range(ROW):
            high_s[g] = jnp.full((1, queries), -1e30, F32)
            total_s[g] = jnp.zeros((VROWS, queries), F32)
        first = scores(0, 0)
        score[0] = first

        def body(u, top):
            stage = lax.div(u, ROW)
            g = lax.rem(u, ROW)

            @pl.when((stage == 0) & (g < ROW - 1))
            def _():
                for k in range(ROW):
                    asked((g + 1) * ROW + k)

            @pl.when((g == ROW - 1) & (stage < ROW - 1))
            def _():
                for k in range(ROW):
                    n = (stage + 1) * ROW + k
                    arrived(n)
                    forward(n).start()

            @pl.when((g == ROW - 1) & (stage >= ROW - 1) & (stage < stages - 1))
            def _():
                for k in range(ROW):
                    forward((stage + 1 - ROW) * ROW + k).wait_recv()

            highest = high_s[g]
            total = total_s[g]
            for slot in range(2):
                raised = jnp.maximum(highest, top)
                fade = jnp.exp2(highest - raised)
                weights = jnp.exp2(score[slot] - raised).astype(BF16)
                if slot == 0:
                    ahead = scores(u, 1)
                else:
                    ahead = scores(jnp.minimum(u + 1, stages * ROW - 1), 0)
                score[1 - slot] = ahead
                top = jnp.max(ahead, axis=0, keepdims=True)
                total = total * fade + jnp.dot(
                    values(u, slot), weights, preferred_element_type=F32
                )
                highest = raised
            high_s[g] = highest
            total_s[g] = total

            @pl.when(stage == stages - 1)
            def _():
                final = total_s[g]
                mixed = (final[0:HEAD] / final[HEAD : HEAD + 1]).astype(BF16)
                row_step = g + jnp.where(g == 2, 1, 0) - jnp.where(g == 3, 1, 0)
                source_row = lax.rem(y + ROW - row_step, ROW)
                for k in range(ROW):
                    n = g * ROW + k
                    o_out[n] = mixed[:, k * tokens : (k + 1) * tokens]
                    source = source_row * ROW + lax.rem(x + ROW - k, ROW)
                    back = remote(
                        o_out.at[n], att.at[here], o_s.at[n], o_r.at[n], half * PLANE + source
                    )
                    if k == 0:

                        @pl.when(g > 0)
                        def _():
                            back.start()
                    else:
                        back.start()

            return top

        lax.fori_loop(0, stages * ROW, body, jnp.max(first, axis=0, keepdims=True))
        att[here] = o_out[0]

        def returned(n):
            head = order[n][2] * ROW + order[n][3]
            return remote(o_out.at[n], att.at[head], o_s.at[n], o_r.at[n], beside)

        for n in range(1, PLANE):
            returned(n).wait_recv()
        loads[0].wait()
        attended = att[...].reshape(width, tokens).T
        stream = (
            resv[...].astype(F32)
            + jnp.dot(attended, wo[...], preferred_element_type=F32)
            + ob_ref[...]
        ).astype(BF16)
        rows = stream.astype(F32)
        normed_two = normalize(rows, g2_ref[...], s2_ref[...]).astype(BF16)
        loads[1].wait()
        loads[2].wait()

        def mlp(c, total):
            at = pl.multiple_of(c * step, step)
            hidden = (
                jnp.dot(normed_two, w1v[:, pl.ds(at, step)], preferred_element_type=F32)
                + b1_ref[:, pl.ds(at, step)]
            )
            hidden = 0.5 * hidden * (1.0 + lax.erf(hidden * math.sqrt(0.5)))
            return total + jnp.dot(
                hidden.astype(BF16), w2v[pl.ds(at, step), :], preferred_element_type=F32
            )

        out_ref[...] = lax.fori_loop(0, hidden_width // step, mlp, rows + b2_ref[...]).astype(BF16)
        for n in range(1, PLANE):
            q_copy(n).wait_send()
            kv_copy(n).wait_send()
            returned(n).wait_send()
        for n in range(PLANE):
            forward(n).wait_send()

    vmem = pl.BlockSpec(memory_space=pltpu.VMEM)
    anywhere = pl.BlockSpec(memory_space=pl.ANY)
    dma = pltpu.SemaphoreType.DMA
    return pl.pallas_call(
        kernel,
        in_specs=[
            vmem, vmem, vmem, anywhere, vmem, vmem, anywhere, vmem,
            anywhere, vmem, vmem, vmem, anywhere, vmem, anywhere, vmem,
        ],
        out_specs=vmem,
        out_shape=jax.ShapeDtypeStruct((tokens, width), BF16),
        scratch_shapes=[
            pltpu.VMEM((8, 128), F32),
            pltpu.VMEM((count - 1, 8, 128), F32),
            pltpu.VMEM((2, side, side), F32),
            pltpu.VMEM((6 * pad, 128), F32),
            pltpu.VMEM((tokens, 6 * 128), BF16),
            pltpu.VMEM((6 * 128, width), BF16),
            pltpu.VMEM(w_qkv.shape, BF16),
            pltpu.VMEM(pos.shape, BF16),
            pltpu.VMEM(w_out.shape, BF16),
            pltpu.VMEM(w1.shape, BF16),
            pltpu.VMEM(w2.shape, BF16),
            pltpu.VMEM((tokens, width), BF16),
            pltpu.VMEM((HEADS, HEAD, tokens), BF16),
            pltpu.VMEM((HEADS, 256, 128), BF16),
            pltpu.VMEM((PLANE, 3 * HEAD, tokens), BF16),
            pltpu.VMEM((2 * PLANE, 256, 128), BF16),
            pltpu.VMEM((2, chunk, queries), F32),
            pltpu.VMEM((ROW, 1, queries), F32),
            pltpu.VMEM((ROW, VROWS, queries), F32),
            pltpu.VMEM((PLANE, HEAD, tokens), BF16),
            pltpu.VMEM((HEADS, HEAD, tokens), BF16),
            dma((count - 1,)), dma((count - 1,)), dma((2,)), dma((2,)),
            dma((PLANE,)), dma((PLANE,)), dma((PLANE,)), dma((PLANE,)),
            dma((PLANE,)), dma((PLANE,)), dma((PLANE,)), dma((PLANE,)), dma((5,)),
        ],
        compiler_params=pltpu.CompilerParams(
            vmem_limit_bytes=VMEM_LIMIT, collective_id=0, has_side_effects=True
        ),
        name="encoder",
    )(
        density, stem_weight, stem_bias, pos, gain1, shift1, w_qkv, qkv_bias,
        w_out, out_bias, gain2, shift2, w1, b1, w2, b2,
    )


def per_device(
    density, stem_weight, stem_bias, pos_embed, ln1_gain, ln1_bias, w_qkv, qkv_bias,
    w_out, out_bias, ln2_gain, ln2_bias, w_fc1, fc1_bias, w_fc2, fc2_bias,
):
    def flat(vector):
        return vector.reshape(1, -1)

    return encoder(
        density, stem_weight, flat(stem_bias), pos_embed, flat(ln1_gain), flat(ln1_bias),
        w_qkv, flat(qkv_bias), w_out, flat(out_bias), flat(ln2_gain), flat(ln2_bias),
        w_fc1, flat(fc1_bias), w_fc2, flat(fc2_bias),
        float(density.size * lax.axis_size("ctx")),
    )


def solution(mesh):
    in_specs = (P(("dp", "ctx"), None, None), P(), P(), P("ctx", None)) + (P(),) * 12
    return jax.shard_map(
        per_device, mesh=mesh, in_specs=in_specs, out_specs=P(("dp", "ctx"), None), check_vma=False
    )
```

```python
import math

import jax
import jax.numpy as jnp
from jax import lax
from jax.experimental import pallas as pl
from jax.experimental.pallas import tpu as pltpu
from jax.sharding import PartitionSpec as P

F32 = jnp.float32
BF16 = jnp.bfloat16
HEADS = 16
HEAD = 64
VROWS = 80
PLANE = 16
ROW = 4
MESH = pl.DeviceIdType.MESH
VMEM_LIMIT = 58 * 2**20


def remote(src, dst, send, recv, index):
    return pltpu.make_async_remote_copy(
        src_ref=src,
        dst_ref=dst,
        send_sem=send,
        recv_sem=recv,
        device_id={"ctx": index},
        device_id_type=MESH,
    )


def greet(peers):
    barrier = pltpu.get_barrier_semaphore()
    for peer in peers:
        pl.semaphore_signal(barrier, inc=1, device_id={"ctx": peer}, device_id_type=MESH)
    return barrier


def normalize(rows, gain, shift):
    center = rows - jnp.mean(rows, axis=-1, keepdims=True)
    spread = jnp.mean(center * center, axis=-1, keepdims=True)
    return center * lax.rsqrt(spread + 1e-06) * gain + shift


def plane_order(me):
    y, x = lax.rem(lax.div(me, ROW), ROW), lax.rem(me, ROW)
    order = []
    for i in (0, 1, 3, 2):
        for j in range(ROW):
            order.append((i, j, lax.rem(y + i, ROW), lax.rem(x + j, ROW)))
    return order


def encoder(
    density, stem_weight, stem_bias, pos, gain1, shift1, w_qkv, qkv_bias,
    w_out, out_bias, gain2, shift2, w1, b1, w2, b2, cells,
):
    planes, side, _ = density.shape
    count = lax.axis_size("ctx")
    width = stem_weight.shape[1]
    hidden_width = w1.shape[1]
    tokens = pos.shape[0]
    grid = side // 4
    lanes = grid * 128
    scale = math.log2(math.e) / math.sqrt(HEAD)
    pad = 72
    stages = 2 * ROW
    group = 2 * ROW
    queries = group * tokens
    chunk = 2 * tokens
    strip = 512
    step = 512

    def kernel(
        d_ref, ws_ref, sb_ref, pos_ref, g1_ref, s1_ref, wq_ref, qb_ref,
        wo_ref, ob_ref, g2_ref, s2_ref, w1_ref, b1_ref, w2_ref, b2_ref,
        out_ref,
        mine, sums, halo, fp, x6, w6, wq, posv, wo, w1v, w2v, resv,
        q_out, kv_out, q_in, kv_in, score, high_s, total_s, o_out, att,
        sum_s, sum_r, halo_s, halo_r, q_s, q_r, kv_s, kv_r, f_s, f_r, o_s, o_r, load,
    ):
        me = lax.axis_index("ctx")
        half = lax.div(me, PLANE)
        here = lax.rem(me, PLANE)
        y, x = lax.div(here, ROW), lax.rem(here, ROW)
        beside = (1 - half) * PLANE + here
        peers = [lax.rem(me + i, count) for i in range(1, count)]
        barrier = greet(peers)
        load_w = pltpu.make_async_copy(wq_ref, wq, load.at[0])
        load_w.start()
        load_p = pltpu.make_async_copy(pos_ref, posv, load.at[1])
        load_p.start()

        slab = d_ref[...]
        part = jnp.sum(slab, axis=0)
        part = jnp.sum(part, axis=0, keepdims=True)
        part = jnp.sum(part, axis=1, keepdims=True)
        mine[...] = jnp.broadcast_to(part, (8, 128))
        fp[...] = jnp.zeros(fp.shape, F32)
        w6[...] = jnp.zeros(w6.shape, BF16)
        for a in range(6):
            w6[a * 128 : a * 128 + 36, :] = ws_ref[a * 36 : (a + 1) * 36, :]
        pl.semaphore_wait(barrier, count - 1)

        up, down = peers[0], peers[-1]
        to_up = remote(d_ref.at[planes - 1], halo.at[0], halo_s.at[0], halo_r.at[0], up)
        to_down = remote(d_ref.at[0], halo.at[1], halo_s.at[1], halo_r.at[1], down)
        to_up.start()
        to_down.start()
        shares = []
        for i, peer in enumerate(peers):
            shares.append(remote(mine, sums.at[i], sum_s.at[i], sum_r.at[i], peer))
            shares[-1].start()
        for i in range(PLANE):
            q_in[i, 0:HEAD, :] = jnp.zeros((HEAD, tokens), BF16)
            q_in[i, 2 * HEAD : 3 * HEAD, :] = jnp.zeros((HEAD, tokens), BF16)
        for share in shares:
            share.wait()
        to_up.wait()
        to_down.wait()
        total = mine[...] + jnp.sum(sums[...], axis=0)
        mean = (total / cells)[0:1, 0:1]

        def logged(values):
            return jnp.log(values / mean).astype(BF16).astype(F32)

        low = jnp.where(me > 0, logged(halo[0]), 0.0)
        high = jnp.where(me < count - 1, logged(halo[1]), 0.0)
        own = logged(slab.reshape(planes * side, side))
        fp[1 : 1 + side, 0:side] = low
        for a in range(planes):
            at = (a + 1) * pad + 1
            fp[at : at + side, 0:side] = own[a * side : (a + 1) * side, :]
        at = (planes + 1) * pad + 1
        fp[at : at + side, 0:side] = high

        z = lax.broadcasted_iota(jnp.int32, (side, lanes), 0)
        col = lax.broadcasted_iota(jnp.int32, (side, lanes), 1)
        lane = jnp.bitwise_and(col, 127)
        base = z + 1 - 4 * jnp.right_shift(col, 7) - lane
        spread = jnp.zeros((6 * grid, lanes), F32)
        for b in range(6):
            rows = jnp.concatenate(
                [fp[pl.ds(a * pad + b, grid, stride=4), 0:side] for a in range(6)], axis=0
            )
            pick = (base == -6 * b) & (lane >= 6 * b) & (lane < 6 * b + 6)
            spread += jnp.dot(
                rows.astype(BF16),
                jnp.where(pick, 1.0, 0.0).astype(BF16),
                preferred_element_type=F32,
            )
        spread = spread.astype(BF16)
        for k in range(grid):
            for a in range(6):
                x6[k * grid : (k + 1) * grid, a * 128 : (a + 1) * 128] = spread[
                    a * grid : (a + 1) * grid, k * 128 : (k + 1) * 128
                ]
        r = lax.broadcasted_iota(jnp.int32, (tokens, tokens), 0)
        s = lax.broadcasted_iota(jnp.int32, (tokens, tokens), 1)
        turn = (jnp.right_shift(r, 4) == jnp.bitwise_and(s, 15)) & (
            jnp.bitwise_and(r, 15) == jnp.right_shift(s, 4)
        )
        patches = jnp.dot(
            jnp.where(turn, 1.0, 0.0).astype(BF16), x6[...], preferred_element_type=F32
        ).astype(BF16)
        load_p.wait()
        embedded = (
            jnp.dot(patches, w6[...], preferred_element_type=F32)
            + sb_ref[...]
            + posv[...].astype(F32)
        )
        residual = embedded.astype(BF16)
        resv[...] = residual
        normed = normalize(residual.astype(F32), g1_ref[...], s1_ref[...]).astype(BF16)

        load_w.wait()
        loads = [
            pltpu.make_async_copy(wo_ref, wo, load.at[2]),
            pltpu.make_async_copy(w1_ref, w1v, load.at[3]),
            pltpu.make_async_copy(w2_ref, w2v, load.at[4]),
        ]
        left = lax.broadcasted_iota(jnp.int32, (128, 128), 1) < HEAD
        order = plane_order(me)

        def project(part_index, row):
            at = pl.multiple_of(part_index * width + row * 256, 256)
            return (
                jnp.dot(normed, wq[:, pl.ds(at, 256)], preferred_element_type=F32)
                + qb_ref[:, pl.ds(at, 256)]
            )

        def make_q(row):
            turned = (project(0, row) * scale).T.astype(BF16)
            for k in range(ROW):
                q_out[row * ROW + k] = turned[k * HEAD : (k + 1) * HEAD, :]

        def make_kv(row):
            keys = project(1, row)
            turned = project(2, row).T.astype(BF16)
            for k in range(ROW):
                pair = keys[:, (k // 2) * 128 : (k // 2 + 1) * 128]
                lo, hi = pair[0:128], pair[128:256]
                if k % 2 == 0:
                    packed = jnp.where(left, lo, pltpu.roll(hi, HEAD, 1))
                else:
                    packed = jnp.where(left, pltpu.roll(lo, HEAD, 1), hi)
                at = row * ROW + k
                kv_out[at, 0:128, :] = packed.astype(BF16)
                kv_out[at, 128 : 128 + HEAD, :] = turned[k * HEAD : (k + 1) * HEAD, 0:128]
                kv_out[at, 128 + HEAD : 256, :] = turned[k * HEAD : (k + 1) * HEAD, 128:256]

        def q_copy(n):
            head = order[n][2] * ROW + order[n][3]
            return remote(
                q_out.at[head], q_in.at[n, HEAD : 2 * HEAD], q_s.at[n], q_r.at[n], half * PLANE + head
            )

        def kv_copy(n):
            head = order[n][2] * ROW + order[n][3]
            return remote(kv_out.at[head], kv_in.at[n], kv_s.at[n], kv_r.at[n], half * PLANE + head)

        make_kv(order[0][2])
        kv_in[0] = kv_out[here]
        for n in range(1, ROW):
            kv_copy(n).start()
        remote(kv_out.at[here], kv_in.at[PLANE], f_s.at[0], f_r.at[0], beside).start()
        for g in range(ROW):
            make_q(order[g * ROW][2])
            for n in range(g * ROW, (g + 1) * ROW):
                if n:
                    q_copy(n).start()
        q_in[0, HEAD : 2 * HEAD, :] = q_out[here]
        for g in range(1, ROW):
            make_kv(order[g * ROW][2])

        def forward(n):
            return remote(kv_in.at[n], kv_in.at[PLANE + n], f_s.at[n], f_r.at[n], beside)

        def arrived(n):
            remote(kv_in.at[n], kv_in.at[n], kv_s.at[n], kv_r.at[n], beside).wait_recv()

        def asked(n):
            remote(
                q_in.at[n, HEAD : 2 * HEAD], q_in.at[n, HEAD : 2 * HEAD], q_s.at[n], q_r.at[n], beside
            ).wait_recv()

        for n in range(1, ROW):
            arrived(n)
            forward(n).start()
        for n in range(1, ROW):
            kv_copy(n).wait_send()
        for n in range(1, PLANE):
            q_copy(n).wait_send()
        for n in range(ROW, 3 * ROW):
            kv_copy(n).start()
        for copy in loads:
            copy.start()
        for n in range(1, PLANE):
            asked(n)

        ones = jnp.where(
            lax.broadcasted_iota(jnp.int32, (VROWS - HEAD, 128), 0) == 0, 1.0, 0.0
        ).astype(BF16)

        def place(it, uu):
            late = it >= stages - 2
            stage = jnp.where(late, stages - 2 + uu, it)
            g = jnp.where(late, it - (stages - 2), uu)
            return stage, g

        def scores(spot, c, h, upper):
            stage, g = spot
            keys = kv_in[pl.ds(stage * ROW + 2 * c, 2), 0:128, :].reshape(256, 128)
            at = 0 if upper else HEAD
            asking = jnp.concatenate(
                [q_in[g * group + 2 * h + k, at : at + 128, :] for k in range(2)], axis=1
            )
            return jnp.dot(keys, asking, preferred_element_type=F32)

        def values(spot, c):
            n = spot[0] * ROW + 2 * c
            pieces = []
            for at in (128, 128 + HEAD):
                for k in range(2):
                    pieces.append(
                        jnp.concatenate([kv_in[n + k, at : at + HEAD, :], ones], axis=0)
                    )
            return jnp.concatenate(pieces, axis=1)

        for g in range(2):
            high_s[g] = jnp.full((1, queries), -1e30, F32)
            total_s[g] = jnp.zeros((VROWS, queries), F32)

        def ahead(slot, spot, c, h):
            top = None
            span = slice(h * strip, (h + 1) * strip)
            for upper in range(2):
                piece = scores(spot, c, h, upper)
                score[slot, upper * 256 : (upper + 1) * 256, span] = piece
                piece = jnp.max(piece, axis=0, keepdims=True)
                top = piece if top is None else jnp.maximum(top, piece)
            return top

        def take(stage):
            for k in range(ROW):
                arrived(stage * ROW + k)
                forward(stage * ROW + k).start()

        def take_beside(stage):
            for k in range(ROW):
                forward(stage * ROW + k).wait_recv()

        def body(it, top):
            for uu in range(2):
                spot = place(it, uu)
                g = spot[1]
                highest = high_s[g]
                total = total_s[g]
                for c in range(2):
                    if c == 1 and uu == 0:

                        @pl.when(it == stages - 2)
                        def _():
                            take_beside(ROW - 1)

                    if c == 1 and uu == 1:

                        @pl.when(it == 0)
                        def _():
                            for n in range(ROW, 3 * ROW):
                                kv_copy(n).wait_send()
                            for n in range(3 * ROW, PLANE):
                                kv_copy(n).start()

                        @pl.when(it < ROW - 1)
                        def _():
                            take(it + 1)

                        @pl.when((it >= ROW - 1) & (it < stages - 2))
                        def _():
                            take_beside(it - (ROW - 1))

                    if c == 0:
                        after, c_after = spot, 1
                    elif uu == 0:
                        after, c_after = place(it, 1), 0
                    else:
                        after, c_after = place(jnp.minimum(it + 1, stages - 1), 0), 0
                    raised = jnp.maximum(highest, top)
                    fade = jnp.exp2(highest - raised)
                    values_now = values(spot, c)
                    tops, totals = [], []
                    for h in range(queries // strip):
                        span = slice(h * strip, (h + 1) * strip)
                        piece = total[:, span] * fade[:, span]
                        best = None
                        for upper in range(2):
                            rows = slice(upper * 256, (upper + 1) * 256)
                            coming = scores(after, c_after, h, upper)
                            weights = jnp.exp2(score[c, rows, span] - raised[:, span]).astype(BF16)
                            score[1 - c, rows, span] = coming
                            coming = jnp.max(coming, axis=0, keepdims=True)
                            best = coming if best is None else jnp.maximum(best, coming)
                            piece = piece + jnp.dot(
                                values_now[:, rows], weights, preferred_element_type=F32
                            )
                        tops.append(best)
                        totals.append(piece)
                    top = jnp.concatenate(tops, axis=1)
                    total = jnp.concatenate(totals, axis=1)
                    highest = raised
                high_s[g] = highest
                total_s[g] = total

            @pl.when(it >= stages - 2)
            def _():
                g = it - (stages - 2)
                final = total_s[g]
                mixed = (final[0:HEAD] / final[HEAD : HEAD + 1]).astype(BF16)
                for r in range(2):
                    row_step = jnp.where(g == 0, r, 3 - r)
                    source_row = lax.rem(y + ROW - row_step, ROW)
                    for k in range(ROW):
                        n = g * group + r * ROW + k
                        at = (r * ROW + k) * tokens
                        o_out[n] = mixed[:, at : at + tokens]
                        source = source_row * ROW + lax.rem(x + ROW - k, ROW)
                        back = remote(
                            o_out.at[n], att.at[here], o_s.at[n], o_r.at[n], half * PLANE + source
                        )
                        if r == 0 and k == 0:

                            @pl.when(g > 0)
                            def _():
                                back.start()
                        else:
                            back.start()

            return top

        top = jnp.concatenate(
            [ahead(0, (0, 0), 0, h) for h in range(queries // strip)], axis=1
        )
        lax.fori_loop(0, stages, body, top)
        att[here] = o_out[0]

        def returned(n):
            head = order[n][2] * ROW + order[n][3]
            return remote(o_out.at[n], att.at[head], o_s.at[n], o_r.at[n], beside)

        for n in range(1, PLANE):
            returned(n).wait_recv()
        loads[0].wait()
        attended = att[...].reshape(width, tokens).T
        stream = (
            resv[...].astype(F32)
            + jnp.dot(attended, wo[...], preferred_element_type=F32)
            + ob_ref[...]
        ).astype(BF16)
        rows = stream.astype(F32)
        normed_two = normalize(rows, g2_ref[...], s2_ref[...]).astype(BF16)
        loads[1].wait()
        loads[2].wait()

        def expand(c):
            span = slice(c * step, (c + 1) * step)
            return (
                jnp.dot(normed_two, w1v[:, span], preferred_element_type=F32) + b1_ref[:, span]
            )

        total = rows + b2_ref[...]
        coming = expand(0)
        for c in range(hidden_width // step):
            hidden = coming
            if c + 1 < hidden_width // step:
                coming = expand(c + 1)
            hidden = 0.5 * hidden * (1.0 + lax.erf(hidden * math.sqrt(0.5)))
            total = total + jnp.dot(
                hidden.astype(BF16), w2v[c * step : (c + 1) * step, :], preferred_element_type=F32
            )
        out_ref[...] = total.astype(BF16)
        for n in range(1, PLANE):
            returned(n).wait_send()
        for n in range(3 * ROW, PLANE):
            kv_copy(n).wait_send()
        for n in range(PLANE):
            forward(n).wait_send()

    vmem = pl.BlockSpec(memory_space=pltpu.VMEM)
    anywhere = pl.BlockSpec(memory_space=pl.ANY)
    dma = pltpu.SemaphoreType.DMA
    return pl.pallas_call(
        kernel,
        in_specs=[
            vmem, vmem, vmem, anywhere, vmem, vmem, anywhere, vmem,
            anywhere, vmem, vmem, vmem, anywhere, vmem, anywhere, vmem,
        ],
        out_specs=vmem,
        out_shape=jax.ShapeDtypeStruct((tokens, width), BF16),
        scratch_shapes=[
            pltpu.VMEM((8, 128), F32),
            pltpu.VMEM((count - 1, 8, 128), F32),
            pltpu.VMEM((2, side, side), F32),
            pltpu.VMEM((6 * pad, 128), F32),
            pltpu.VMEM((tokens, 6 * 128), BF16),
            pltpu.VMEM((6 * 128, width), BF16),
            pltpu.VMEM(w_qkv.shape, BF16),
            pltpu.VMEM(pos.shape, BF16),
            pltpu.VMEM(w_out.shape, BF16),
            pltpu.VMEM(w1.shape, BF16),
            pltpu.VMEM(w2.shape, BF16),
            pltpu.VMEM((tokens, width), BF16),
            pltpu.VMEM((HEADS, HEAD, tokens), BF16),
            pltpu.VMEM((HEADS, 256, 128), BF16),
            pltpu.VMEM((PLANE, 3 * HEAD, tokens), BF16),
            pltpu.VMEM((2 * PLANE, 256, 128), BF16),
            pltpu.VMEM((2, chunk, queries), F32),
            pltpu.VMEM((2, 1, queries), F32),
            pltpu.VMEM((2, VROWS, queries), F32),
            pltpu.VMEM((PLANE, HEAD, tokens), BF16),
            pltpu.VMEM((HEADS, HEAD, tokens), BF16),
            dma((count - 1,)), dma((count - 1,)), dma((2,)), dma((2,)),
            dma((PLANE,)), dma((PLANE,)), dma((PLANE,)), dma((PLANE,)),
            dma((PLANE,)), dma((PLANE,)), dma((PLANE,)), dma((PLANE,)), dma((5,)),
        ],
        compiler_params=pltpu.CompilerParams(
            vmem_limit_bytes=VMEM_LIMIT, collective_id=0, has_side_effects=True
        ),
        name="encoder",
    )(
        density, stem_weight, stem_bias, pos, gain1, shift1, w_qkv, qkv_bias,
        w_out, out_bias, gain2, shift2, w1, b1, w2, b2,
    )


def per_device(
    density, stem_weight, stem_bias, pos_embed, ln1_gain, ln1_bias, w_qkv, qkv_bias,
    w_out, out_bias, ln2_gain, ln2_bias, w_fc1, fc1_bias, w_fc2, fc2_bias,
):
    def flat(vector):
        return vector.reshape(1, -1)

    return encoder(
        density, stem_weight, flat(stem_bias), pos_embed, flat(ln1_gain), flat(ln1_bias),
        w_qkv, flat(qkv_bias), w_out, flat(out_bias), flat(ln2_gain), flat(ln2_bias),
        w_fc1, flat(fc1_bias), w_fc2, flat(fc2_bias),
        float(density.size * lax.axis_size("ctx")),
    )


def solution(mesh):
    in_specs = (P(("dp", "ctx"), None, None), P(), P(), P("ctx", None)) + (P(),) * 12
    return jax.shard_map(
        per_device, mesh=mesh, in_specs=in_specs, out_specs=P(("dp", "ctx"), None), check_vma=False
    )
```

```python
import math

import jax
import jax.numpy as jnp
from jax import lax
from jax.experimental import pallas as pl
from jax.experimental.pallas import tpu as pltpu
from jax.sharding import PartitionSpec as P

F32 = jnp.float32
BF16 = jnp.bfloat16
HEADS = 16
HEAD = 64
VROWS = 80
PLANE = 16
ROW = 4
MESH = pl.DeviceIdType.MESH
VMEM_LIMIT = 58 * 2**20


def remote(src, dst, send, recv, index):
    return pltpu.make_async_remote_copy(
        src_ref=src,
        dst_ref=dst,
        send_sem=send,
        recv_sem=recv,
        device_id={"ctx": index},
        device_id_type=MESH,
    )


def greet(peers):
    barrier = pltpu.get_barrier_semaphore()
    for peer in peers:
        pl.semaphore_signal(barrier, inc=1, device_id={"ctx": peer}, device_id_type=MESH)
    return barrier


def normalize(rows, gain, shift):
    center = rows - jnp.mean(rows, axis=-1, keepdims=True)
    spread = jnp.mean(center * center, axis=-1, keepdims=True)
    return center * lax.rsqrt(spread + 1e-06) * gain + shift


def plane_order(me):
    y, x = lax.rem(lax.div(me, ROW), ROW), lax.rem(me, ROW)
    order = []
    for i in (0, 1, 3, 2):
        for j in range(ROW):
            order.append((i, j, lax.rem(y + i, ROW), lax.rem(x + j, ROW)))
    return order


def encoder(
    density, stem_weight, stem_bias, pos, gain1, shift1, w_qkv, qkv_bias,
    w_out, out_bias, gain2, shift2, w1, b1, w2, b2, cells,
):
    planes, side, _ = density.shape
    count = lax.axis_size("ctx")
    width = stem_weight.shape[1]
    hidden_width = w1.shape[1]
    tokens = pos.shape[0]
    grid = side // 4
    lanes = grid * 128
    scale = math.log2(math.e) / math.sqrt(HEAD)
    pad = 72
    stages = 2 * ROW
    group = 2 * ROW
    queries = group * tokens
    chunk = 2 * tokens
    strip = 512
    step = 512

    def kernel(
        d_hbm, ws_hbm, sb_hbm, pos_ref, g1_hbm, s1_hbm, wq_ref, qb_hbm,
        wo_ref, ob_hbm, g2_hbm, s2_hbm, w1_ref, b1_hbm, w2_ref, b2_hbm,
        out_ref,
        d_ref, ws_ref, sb_ref, g1_ref, s1_ref, qb_ref, ob_ref, g2_ref, s2_ref, b1_ref, b2_ref,
        mine, sums, halo, fp, x6, w6, wq, posv, wo, w1v, w2v, resv,
        q_out, kv_out, q_in, kv_in, score, high_s, total_s, o_out, att,
        sum_s, sum_r, halo_s, halo_r, q_s, q_r, kv_s, kv_r, f_s, f_r, o_s, o_r, load,
    ):
        me = lax.axis_index("ctx")
        half = lax.div(me, PLANE)
        here = lax.rem(me, PLANE)
        y, x = lax.div(here, ROW), lax.rem(here, ROW)
        beside = (1 - half) * PLANE + here
        peers = [lax.rem(me + i, count) for i in range(1, count)]
        barrier = greet(peers)
        load_w = pltpu.make_async_copy(wq_ref, wq, load.at[0])
        load_p = pltpu.make_async_copy(pos_ref, posv, load.at[1])

        small = [
            pltpu.make_async_copy(source, target, load.at[5 + i])
            for i, (source, target) in enumerate(
                (
                    (d_hbm, d_ref), (ws_hbm, ws_ref), (sb_hbm, sb_ref), (g1_hbm, g1_ref),
                    (s1_hbm, s1_ref), (qb_hbm, qb_ref), (ob_hbm, ob_ref), (g2_hbm, g2_ref),
                    (s2_hbm, s2_ref), (b1_hbm, b1_ref), (b2_hbm, b2_ref),
                )
            )
        ]
        for copy in small:
            copy.start()
        load_w.start()
        load_p.start()
        small[0].wait()
        slab = d_ref[...]
        part = jnp.sum(slab, axis=0)
        part = jnp.sum(part, axis=0, keepdims=True)
        part = jnp.sum(part, axis=1, keepdims=True)
        mine[...] = jnp.broadcast_to(part, (8, 128))
        fp[...] = jnp.zeros(fp.shape, F32)
        w6[...] = jnp.zeros(w6.shape, BF16)
        for copy in small[1:]:
            copy.wait()
        for a in range(6):
            w6[a * 128 : a * 128 + 36, :] = ws_ref[a * 36 : (a + 1) * 36, :]
        pl.semaphore_wait(barrier, count - 1)

        up, down = peers[0], peers[-1]
        to_up = remote(d_ref.at[planes - 1], halo.at[0], halo_s.at[0], halo_r.at[0], up)
        to_down = remote(d_ref.at[0], halo.at[1], halo_s.at[1], halo_r.at[1], down)
        to_up.start()
        to_down.start()
        shares = []
        for i, peer in enumerate(peers):
            shares.append(remote(mine, sums.at[i], sum_s.at[i], sum_r.at[i], peer))
            shares[-1].start()
        for i in range(PLANE):
            q_in[i, 0:HEAD, :] = jnp.zeros((HEAD, tokens), BF16)
            q_in[i, 2 * HEAD : 3 * HEAD, :] = jnp.zeros((HEAD, tokens), BF16)
        for share in shares:
            share.wait()
        to_up.wait()
        to_down.wait()
        total = mine[...] + jnp.sum(sums[...], axis=0)
        mean = (total / cells)[0:1, 0:1]

        def logged(values):
            return jnp.log(values / mean).astype(BF16).astype(F32)

        low = jnp.where(me > 0, logged(halo[0]), 0.0)
        high = jnp.where(me < count - 1, logged(halo[1]), 0.0)
        own = logged(slab.reshape(planes * side, side))
        fp[1 : 1 + side, 0:side] = low
        for a in range(planes):
            at = (a + 1) * pad + 1
            fp[at : at + side, 0:side] = own[a * side : (a + 1) * side, :]
        at = (planes + 1) * pad + 1
        fp[at : at + side, 0:side] = high

        z = lax.broadcasted_iota(jnp.int32, (side, lanes), 0)
        col = lax.broadcasted_iota(jnp.int32, (side, lanes), 1)
        lane = jnp.bitwise_and(col, 127)
        base = z + 1 - 4 * jnp.right_shift(col, 7) - lane
        spread = jnp.zeros((6 * grid, lanes), F32)
        for b in range(6):
            rows = jnp.concatenate(
                [fp[pl.ds(a * pad + b, grid, stride=4), 0:side] for a in range(6)], axis=0
            )
            pick = (base == -6 * b) & (lane >= 6 * b) & (lane < 6 * b + 6)
            spread += jnp.dot(
                rows.astype(BF16),
                jnp.where(pick, 1.0, 0.0).astype(BF16),
                preferred_element_type=F32,
            )
        spread = spread.astype(BF16)
        for k in range(grid):
            for a in range(6):
                x6[k * grid : (k + 1) * grid, a * 128 : (a + 1) * 128] = spread[
                    a * grid : (a + 1) * grid, k * 128 : (k + 1) * 128
                ]
        r = lax.broadcasted_iota(jnp.int32, (tokens, tokens), 0)
        s = lax.broadcasted_iota(jnp.int32, (tokens, tokens), 1)
        turn = (jnp.right_shift(r, 4) == jnp.bitwise_and(s, 15)) & (
            jnp.bitwise_and(r, 15) == jnp.right_shift(s, 4)
        )
        patches = jnp.dot(
            jnp.where(turn, 1.0, 0.0).astype(BF16), x6[...], preferred_element_type=F32
        ).astype(BF16)
        load_p.wait()
        embedded = (
            jnp.dot(patches, w6[...], preferred_element_type=F32)
            + sb_ref[...]
            + posv[...].astype(F32)
        )
        residual = embedded.astype(BF16)
        resv[...] = residual
        normed = normalize(residual.astype(F32), g1_ref[...], s1_ref[...]).astype(BF16)

        load_w.wait()
        loads = [
            pltpu.make_async_copy(wo_ref, wo, load.at[2]),
            pltpu.make_async_copy(w1_ref, w1v, load.at[3]),
            pltpu.make_async_copy(w2_ref, w2v, load.at[4]),
        ]
        left = lax.broadcasted_iota(jnp.int32, (128, 128), 1) < HEAD
        order = plane_order(me)

        def project(part_index, row):
            at = pl.multiple_of(part_index * width + row * 256, 256)
            return (
                jnp.dot(normed, wq[:, pl.ds(at, 256)], preferred_element_type=F32)
                + qb_ref[:, pl.ds(at, 256)]
            )

        def make_q(row):
            turned = (project(0, row) * scale).T.astype(BF16)
            for k in range(ROW):
                q_out[row * ROW + k] = turned[k * HEAD : (k + 1) * HEAD, :]

        def make_kv(row):
            keys = project(1, row)
            turned = project(2, row).T.astype(BF16)
            for k in range(ROW):
                pair = keys[:, (k // 2) * 128 : (k // 2 + 1) * 128]
                lo, hi = pair[0:128], pair[128:256]
                if k % 2 == 0:
                    packed = jnp.where(left, lo, pltpu.roll(hi, HEAD, 1))
                else:
                    packed = jnp.where(left, pltpu.roll(lo, HEAD, 1), hi)
                at = row * ROW + k
                kv_out[at, 0:128, :] = packed.astype(BF16)
                kv_out[at, 128 : 128 + HEAD, :] = turned[k * HEAD : (k + 1) * HEAD, 0:128]
                kv_out[at, 128 + HEAD : 256, :] = turned[k * HEAD : (k + 1) * HEAD, 128:256]

        def q_copy(n):
            head = order[n][2] * ROW + order[n][3]
            return remote(
                q_out.at[head], q_in.at[n, HEAD : 2 * HEAD], q_s.at[n], q_r.at[n], half * PLANE + head
            )

        def kv_copy(n):
            head = order[n][2] * ROW + order[n][3]
            return remote(kv_out.at[head], kv_in.at[n], kv_s.at[n], kv_r.at[n], half * PLANE + head)

        def send_kv(g):
            make_kv(order[g * ROW][2])
            for n in range(g * ROW, (g + 1) * ROW):
                if n:
                    kv_copy(n).start()

        def send_q(g):
            make_q(order[g * ROW][2])
            for n in range(g * ROW, (g + 1) * ROW):
                if n:
                    q_copy(n).start()

        send_kv(0)
        remote(kv_out.at[here], kv_in.at[PLANE], f_s.at[0], f_r.at[0], beside).start()
        for g in range(ROW):
            send_q(g)
        for g in range(1, ROW):
            send_kv(g)
        kv_in[0] = kv_out[here]
        q_in[0, HEAD : 2 * HEAD, :] = q_out[here]

        def forward(n):
            return remote(kv_in.at[n], kv_in.at[PLANE + n], f_s.at[n], f_r.at[n], beside)

        def arrived(n):
            remote(kv_in.at[n], kv_in.at[n], kv_s.at[n], kv_r.at[n], beside).wait_recv()

        def asked(n):
            remote(
                q_in.at[n, HEAD : 2 * HEAD], q_in.at[n, HEAD : 2 * HEAD], q_s.at[n], q_r.at[n], beside
            ).wait_recv()

        for n in range(1, ROW):
            arrived(n)
            forward(n).start()
        for n in range(1, group):
            asked(n)
        for copy in loads:
            copy.start()

        ones = jnp.where(
            lax.broadcasted_iota(jnp.int32, (VROWS - HEAD, 128), 0) == 0, 1.0, 0.0
        ).astype(BF16)

        def scores(spot, c, h, upper):
            stage, g = spot
            keys = kv_in[pl.ds(stage * ROW + 2 * c, 2), 0:128, :].reshape(256, 128)
            at = 0 if upper else HEAD
            asking = jnp.concatenate(
                [q_in[g * group + 2 * h + k, at : at + 128, :] for k in range(2)], axis=1
            )
            return jnp.dot(keys, asking, preferred_element_type=F32)

        def values(spot, c):
            n = spot[0] * ROW + 2 * c
            pieces = []
            for at in (128, 128 + HEAD):
                for k in range(2):
                    pieces.append(
                        jnp.concatenate([kv_in[n + k, at : at + HEAD, :], ones], axis=0)
                    )
            return jnp.concatenate(pieces, axis=1)

        for g in range(2):
            high_s[g] = jnp.full((1, queries), -1e30, F32)
            total_s[g] = jnp.zeros((VROWS, queries), F32)

        def ahead(slot, spot, c, h):
            top = None
            span = slice(h * strip, (h + 1) * strip)
            for upper in range(2):
                piece = scores(spot, c, h, upper)
                score[slot, upper * 256 : (upper + 1) * 256, span] = piece
                piece = jnp.max(piece, axis=0, keepdims=True)
                top = piece if top is None else jnp.maximum(top, piece)
            return top

        def take(stage):
            for k in range(ROW):
                arrived(stage * ROW + k)
                forward(stage * ROW + k).start()

        def take_beside(stage):
            for k in range(ROW):
                forward(stage * ROW + k).wait_recv()

        def advance(spot, c, after, c_after, highest, total, top, finish=None):
            raised = jnp.maximum(highest, top)
            fade = jnp.exp2(highest - raised)
            values_now = values(spot, c)
            tops, totals = [], []
            for h in range(queries // strip):
                span = slice(h * strip, (h + 1) * strip)
                piece = total[:, span] * fade[:, span]
                best = None
                for upper in range(2):
                    rows = slice(upper * 256, (upper + 1) * 256)
                    if after is not None:
                        coming = scores(after, c_after, h, upper)
                    weights = jnp.exp2(score[c, rows, span] - raised[:, span]).astype(BF16)
                    if after is not None:
                        score[1 - c, rows, span] = coming
                        coming = jnp.max(coming, axis=0, keepdims=True)
                        best = coming if best is None else jnp.maximum(best, coming)
                    piece = piece + jnp.dot(
                        values_now[:, rows], weights, preferred_element_type=F32
                    )
                tops.append(best)
                totals.append(piece)
                if finish is not None:
                    finish(spot[1], h, piece)
            if after is not None:
                top = jnp.concatenate(tops, axis=1)
            return raised, jnp.concatenate(totals, axis=1), top

        def body(it, top):
            for g in range(2):
                highest, total = high_s[g], total_s[g]
                highest, total, top = advance((it, g), 0, (it, g), 1, highest, total, top)
                if g == 1:

                    @pl.when(it < ROW - 1)
                    def _():
                        take(it + 1)

                    @pl.when(it >= ROW - 1)
                    def _():
                        take_beside(it - (ROW - 1))

                after = (it, 1) if g == 0 else (it + 1, 0)
                highest, total, top = advance((it, g), 1, after, 0, highest, total, top)
                high_s[g] = highest
                total_s[g] = total
            return top

        def finish(g, h, piece):
            mixed = (piece[0:HEAD] / piece[HEAD : HEAD + 1]).astype(BF16)
            for k in range(2):
                n = g * group + 2 * h + k
                o_out[n] = mixed[:, k * tokens : (k + 1) * tokens]
                if n:
                    i, j = order[n][0], order[n][1]
                    source = lax.rem(y + ROW - i, ROW) * ROW + lax.rem(x + ROW - j, ROW)
                    remote(
                        o_out.at[n], att.at[here], o_s.at[n], o_r.at[n], half * PLANE + source
                    ).start()

        top = jnp.concatenate(
            [ahead(0, (0, 0), 0, h) for h in range(queries // strip)], axis=1
        )
        for g in range(2):
            highest, total, top = advance((0, g), 0, (0, g), 1, high_s[g], total_s[g], top)
            if g == 0:
                for n in range(group, PLANE):
                    asked(n)
            else:
                take(1)
            after = (0, 1) if g == 0 else (1, 0)
            highest, total, top = advance((0, g), 1, after, 0, highest, total, top)
            high_s[g] = highest
            total_s[g] = total
        top = lax.fori_loop(1, stages - 1, body, top)
        last = stages - 1
        for g in range(2):
            highest, total, top = advance(
                (last, g), 0, (last, g), 1, high_s[g], total_s[g], top
            )
            after = (last, 1) if g == 0 else None
            highest, total, top = advance(
                (last, g), 1, after, 0, highest, total, top, finish
            )
        att[here] = o_out[0]

        def returned(n):
            head = order[n][2] * ROW + order[n][3]
            return remote(o_out.at[n], att.at[head], o_s.at[n], o_r.at[n], beside)

        for n in range(1, PLANE):
            returned(n).wait_recv()
        loads[0].wait()
        attended = att[...].reshape(width, tokens).T
        stream = (
            resv[...].astype(F32)
            + jnp.dot(attended, wo[...], preferred_element_type=F32)
            + ob_ref[...]
        ).astype(BF16)
        rows = stream.astype(F32)
        normed_two = normalize(rows, g2_ref[...], s2_ref[...]).astype(BF16)
        loads[1].wait()
        loads[2].wait()

        def expand(c):
            span = slice(c * step, (c + 1) * step)
            return (
                jnp.dot(normed_two, w1v[:, span], preferred_element_type=F32) + b1_ref[:, span]
            )

        total = rows + b2_ref[...]
        coming = expand(0)
        for c in range(hidden_width // step):
            hidden = coming
            if c + 1 < hidden_width // step:
                coming = expand(c + 1)
            hidden = 0.5 * hidden * (1.0 + lax.erf(hidden * math.sqrt(0.5)))
            total = total + jnp.dot(
                hidden.astype(BF16), w2v[c * step : (c + 1) * step, :], preferred_element_type=F32
            )
        out_ref[...] = total.astype(BF16)
        for n in range(1, PLANE):
            returned(n).wait_send()
        for n in range(1, PLANE):
            kv_copy(n).wait_send()
            q_copy(n).wait_send()
        for n in range(PLANE):
            forward(n).wait_send()

    vmem = pl.BlockSpec(memory_space=pltpu.VMEM)
    anywhere = pl.BlockSpec(memory_space=pl.ANY)
    dma = pltpu.SemaphoreType.DMA
    return pl.pallas_call(
        kernel,
        in_specs=[anywhere] * 16,
        out_specs=vmem,
        out_shape=jax.ShapeDtypeStruct((tokens, width), BF16),
        scratch_shapes=[
            pltpu.VMEM(density.shape, F32),
            pltpu.VMEM(stem_weight.shape, BF16),
            pltpu.VMEM(stem_bias.shape, F32),
            pltpu.VMEM(gain1.shape, F32),
            pltpu.VMEM(shift1.shape, F32),
            pltpu.VMEM(qkv_bias.shape, F32),
            pltpu.VMEM(out_bias.shape, F32),
            pltpu.VMEM(gain2.shape, F32),
            pltpu.VMEM(shift2.shape, F32),
            pltpu.VMEM(b1.shape, F32),
            pltpu.VMEM(b2.shape, F32),
            pltpu.VMEM((8, 128), F32),
            pltpu.VMEM((count - 1, 8, 128), F32),
            pltpu.VMEM((2, side, side), F32),
            pltpu.VMEM((6 * pad, 128), F32),
            pltpu.VMEM((tokens, 6 * 128), BF16),
            pltpu.VMEM((6 * 128, width), BF16),
            pltpu.VMEM(w_qkv.shape, BF16),
            pltpu.VMEM(pos.shape, BF16),
            pltpu.VMEM(w_out.shape, BF16),
            pltpu.VMEM(w1.shape, BF16),
            pltpu.VMEM(w2.shape, BF16),
            pltpu.VMEM((tokens, width), BF16),
            pltpu.VMEM((HEADS, HEAD, tokens), BF16),
            pltpu.VMEM((HEADS, 256, 128), BF16),
            pltpu.VMEM((PLANE, 3 * HEAD, tokens), BF16),
            pltpu.VMEM((2 * PLANE, 256, 128), BF16),
            pltpu.VMEM((2, chunk, queries), F32),
            pltpu.VMEM((2, 1, queries), F32),
            pltpu.VMEM((2, VROWS, queries), F32),
            pltpu.VMEM((PLANE, HEAD, tokens), BF16),
            pltpu.VMEM((HEADS, HEAD, tokens), BF16),
            dma((count - 1,)), dma((count - 1,)), dma((2,)), dma((2,)),
            dma((PLANE,)), dma((PLANE,)), dma((PLANE,)), dma((PLANE,)),
            dma((PLANE,)), dma((PLANE,)), dma((PLANE,)), dma((PLANE,)), dma((16,)),
        ],
        compiler_params=pltpu.CompilerParams(
            vmem_limit_bytes=VMEM_LIMIT, collective_id=0, has_side_effects=True
        ),
        name="encoder",
    )(
        density, stem_weight, stem_bias, pos, gain1, shift1, w_qkv, qkv_bias,
        w_out, out_bias, gain2, shift2, w1, b1, w2, b2,
    )


def per_device(
    density, stem_weight, stem_bias, pos_embed, ln1_gain, ln1_bias, w_qkv, qkv_bias,
    w_out, out_bias, ln2_gain, ln2_bias, w_fc1, fc1_bias, w_fc2, fc2_bias,
):
    def flat(vector):
        return vector.reshape(1, -1)

    return encoder(
        density, stem_weight, flat(stem_bias), pos_embed, flat(ln1_gain), flat(ln1_bias),
        w_qkv, flat(qkv_bias), w_out, flat(out_bias), flat(ln2_gain), flat(ln2_bias),
        w_fc1, flat(fc1_bias), w_fc2, flat(fc2_bias),
        float(density.size * lax.axis_size("ctx")),
    )


def solution(mesh):
    in_specs = (P(("dp", "ctx"), None, None), P(), P(), P("ctx", None)) + (P(),) * 12
    return jax.shard_map(
        per_device, mesh=mesh, in_specs=in_specs, out_specs=P(("dp", "ctx"), None), check_vma=False
    )
```

```python
import math

import jax
import jax.numpy as jnp
from jax import lax
from jax.experimental import pallas as pl
from jax.experimental.pallas import tpu as pltpu
from jax.sharding import PartitionSpec as P

F32 = jnp.float32
BF16 = jnp.bfloat16
HEADS = 16
HEAD = 64
VROWS = 80
PLANE = 16
ROW = 4
MESH = pl.DeviceIdType.MESH
VMEM_LIMIT = 58 * 2**20


def remote(src, dst, send, recv, index):
    return pltpu.make_async_remote_copy(
        src_ref=src,
        dst_ref=dst,
        send_sem=send,
        recv_sem=recv,
        device_id={"ctx": index},
        device_id_type=MESH,
    )


def greet(peers):
    barrier = pltpu.get_barrier_semaphore()
    for peer in peers:
        pl.semaphore_signal(barrier, inc=1, device_id={"ctx": peer}, device_id_type=MESH)
    return barrier


def normalize(rows, gain, shift):
    center = rows - jnp.mean(rows, axis=-1, keepdims=True)
    spread = jnp.mean(center * center, axis=-1, keepdims=True)
    return center * lax.rsqrt(spread + 1e-06) * gain + shift


def plane_order(me):
    y, x = lax.rem(lax.div(me, ROW), ROW), lax.rem(me, ROW)
    order = []
    for i in (0, 1, 3, 2):
        for j in range(ROW):
            order.append((i, j, lax.rem(y + i, ROW), lax.rem(x + j, ROW)))
    return order


def encoder(
    density, stem_weight, stem_bias, pos, gain1, shift1, w_qkv, qkv_bias,
    w_out, out_bias, gain2, shift2, w1, b1, w2, b2, cells,
):
    planes, side, _ = density.shape
    count = lax.axis_size("ctx")
    width = stem_weight.shape[1]
    hidden_width = w1.shape[1]
    tokens = pos.shape[0]
    grid = side // 4
    lanes = grid * 128
    scale = math.log2(math.e) / math.sqrt(HEAD)
    pad = 72
    stages = 2 * ROW
    group = 2 * ROW
    queries = group * tokens
    chunk = 2 * tokens
    strip = 512
    step = 512

    def kernel(
        d_hbm, ws_hbm, sb_hbm, pos_ref, g1_hbm, s1_hbm, wq_ref, qb_hbm,
        wo_ref, ob_hbm, g2_hbm, s2_hbm, w1_ref, b1_hbm, w2_ref, b2_hbm,
        out_ref,
        d_ref, ws_ref, sb_ref, g1_ref, s1_ref, qb_ref, ob_ref, g2_ref, s2_ref, b1_ref, b2_ref,
        mine, sums, halo, fp, picks, turned_at, x6, w6, wq, posv, wo, w1v, w2v, resv,
        q_out, kv_out, q_in, kv_in, score, high_s, total_s, o_out, att,
        sum_s, sum_r, halo_s, halo_r, q_s, q_r, kv_s, kv_r, f_s, f_r, o_s, o_r, load,
    ):
        me = lax.axis_index("ctx")
        half = lax.div(me, PLANE)
        here = lax.rem(me, PLANE)
        y, x = lax.div(here, ROW), lax.rem(here, ROW)
        beside = (1 - half) * PLANE + here
        peers = [lax.rem(me + i, count) for i in range(1, count)]
        barrier = greet(peers)
        load_w = pltpu.make_async_copy(wq_ref, wq, load.at[0])
        load_p = pltpu.make_async_copy(pos_ref, posv, load.at[1])

        small = [
            pltpu.make_async_copy(source, target, load.at[5 + i])
            for i, (source, target) in enumerate(
                (
                    (d_hbm, d_ref), (ws_hbm, ws_ref), (sb_hbm, sb_ref), (g1_hbm, g1_ref),
                    (s1_hbm, s1_ref), (qb_hbm, qb_ref), (ob_hbm, ob_ref), (g2_hbm, g2_ref),
                    (s2_hbm, s2_ref), (b1_hbm, b1_ref), (b2_hbm, b2_ref),
                )
            )
        ]
        for copy in small:
            copy.start()
        load_w.start()
        load_p.start()
        small[0].wait()
        slab = d_ref[...]
        part = jnp.sum(slab, axis=0)
        part = jnp.sum(part, axis=0, keepdims=True)
        part = jnp.sum(part, axis=1, keepdims=True)
        mine[...] = jnp.broadcast_to(part, (1, 128))
        fp[...] = jnp.zeros(fp.shape, F32)
        w6[...] = jnp.zeros(w6.shape, BF16)
        for copy in small[1:]:
            copy.wait()
        for a in range(6):
            w6[a * 128 : a * 128 + 36, :] = ws_ref[a * 36 : (a + 1) * 36, :]
        pl.semaphore_wait(barrier, count - 1)

        up, down = peers[0], peers[-1]
        to_up = remote(d_ref.at[planes - 1], halo.at[0], halo_s.at[0], halo_r.at[0], up)
        to_down = remote(d_ref.at[0], halo.at[1], halo_s.at[1], halo_r.at[1], down)
        to_up.start()
        to_down.start()
        shares = []
        for i, peer in enumerate(peers):
            shares.append(remote(mine, sums.at[i], sum_s.at[i], sum_r.at[i], peer))
            shares[-1].start()
        for i in range(PLANE):
            q_in[i, 0:HEAD, :] = jnp.zeros((HEAD, tokens), BF16)
            q_in[i, 2 * HEAD : 3 * HEAD, :] = jnp.zeros((HEAD, tokens), BF16)
        z = lax.broadcasted_iota(jnp.int32, (side, lanes), 0)
        col = lax.broadcasted_iota(jnp.int32, (side, lanes), 1)
        lane = jnp.bitwise_and(col, 127)
        base = z + 1 - 4 * jnp.right_shift(col, 7) - lane
        for b in range(6):
            pick = (base == -6 * b) & (lane >= 6 * b) & (lane < 6 * b + 6)
            picks[b] = jnp.where(pick, 1.0, 0.0).astype(BF16)
        r = lax.broadcasted_iota(jnp.int32, (tokens, tokens), 0)
        s = lax.broadcasted_iota(jnp.int32, (tokens, tokens), 1)
        turn = (jnp.right_shift(r, 4) == jnp.bitwise_and(s, 15)) & (
            jnp.bitwise_and(r, 15) == jnp.right_shift(s, 4)
        )
        turned_at[...] = jnp.where(turn, 1.0, 0.0).astype(BF16)
        for share in shares:
            share.wait()
        to_up.wait()
        to_down.wait()
        total = mine[...] + jnp.sum(sums[...], axis=0)
        mean = (total / cells)[0:1, 0:1]

        def logged(values):
            return jnp.log(values / mean).astype(BF16).astype(F32)

        low = jnp.where(me > 0, logged(halo[0]), 0.0)
        high = jnp.where(me < count - 1, logged(halo[1]), 0.0)
        own = logged(slab.reshape(planes * side, side))
        fp[1 : 1 + side, 0:side] = low
        for a in range(planes):
            at = (a + 1) * pad + 1
            fp[at : at + side, 0:side] = own[a * side : (a + 1) * side, :]
        at = (planes + 1) * pad + 1
        fp[at : at + side, 0:side] = high

        spread = jnp.zeros((6 * grid, lanes), F32)
        for b in range(6):
            rows = jnp.concatenate(
                [fp[pl.ds(a * pad + b, grid, stride=4), 0:side] for a in range(6)], axis=0
            )
            spread += jnp.dot(rows.astype(BF16), picks[b], preferred_element_type=F32)
        spread = spread.astype(BF16)
        for k in range(grid):
            for a in range(6):
                x6[k * grid : (k + 1) * grid, a * 128 : (a + 1) * 128] = spread[
                    a * grid : (a + 1) * grid, k * 128 : (k + 1) * 128
                ]
        patches = jnp.dot(
            turned_at[...], x6[...], preferred_element_type=F32
        ).astype(BF16)
        load_p.wait()
        embedded = (
            jnp.dot(patches, w6[...], preferred_element_type=F32)
            + sb_ref[...]
            + posv[...].astype(F32)
        )
        residual = embedded.astype(BF16)
        resv[...] = residual
        normed = normalize(residual.astype(F32), g1_ref[...], s1_ref[...]).astype(BF16)

        load_w.wait()
        loads = [
            pltpu.make_async_copy(wo_ref, wo, load.at[2]),
            pltpu.make_async_copy(w1_ref, w1v, load.at[3]),
            pltpu.make_async_copy(w2_ref, w2v, load.at[4]),
        ]
        left = lax.broadcasted_iota(jnp.int32, (128, 128), 1) < HEAD
        order = plane_order(me)

        def project(part_index, row):
            at = pl.multiple_of(part_index * width + row * 256, 256)
            return (
                jnp.dot(normed, wq[:, pl.ds(at, 256)], preferred_element_type=F32)
                + qb_ref[:, pl.ds(at, 256)]
            )

        def make_q(row):
            turned = (project(0, row) * scale).astype(BF16).T
            for k in range(ROW):
                q_out[row * ROW + k] = turned[k * HEAD : (k + 1) * HEAD, :]

        def make_kv(row):
            keys = project(1, row)
            turned = project(2, row).astype(BF16).T
            for k in range(ROW):
                pair = keys[:, (k // 2) * 128 : (k // 2 + 1) * 128]
                lo, hi = pair[0:128], pair[128:256]
                if k % 2 == 0:
                    packed = jnp.where(left, lo, pltpu.roll(hi, HEAD, 1))
                else:
                    packed = jnp.where(left, pltpu.roll(lo, HEAD, 1), hi)
                at = row * ROW + k
                kv_out[at, 0:128, :] = packed.astype(BF16)
                kv_out[at, 128 : 128 + HEAD, :] = turned[k * HEAD : (k + 1) * HEAD, 0:128]
                kv_out[at, 128 + HEAD : 256, :] = turned[k * HEAD : (k + 1) * HEAD, 128:256]

        def q_copy(n):
            head = order[n][2] * ROW + order[n][3]
            return remote(
                q_out.at[head], q_in.at[n, HEAD : 2 * HEAD], q_s.at[n], q_r.at[n], half * PLANE + head
            )

        def kv_copy(n):
            head = order[n][2] * ROW + order[n][3]
            return remote(kv_out.at[head], kv_in.at[n], kv_s.at[n], kv_r.at[n], half * PLANE + head)

        def send_kv(g):
            make_kv(order[g * ROW][2])
            for n in range(g * ROW, (g + 1) * ROW):
                if n:
                    kv_copy(n).start()

        def send_q(g):
            make_q(order[g * ROW][2])
            for n in range(g * ROW, (g + 1) * ROW):
                if n:
                    q_copy(n).start()

        send_kv(0)
        remote(kv_out.at[here], kv_in.at[PLANE], f_s.at[0], f_r.at[0], beside).start()
        for g in range(ROW):
            send_q(g)
        for g in range(1, ROW):
            send_kv(g)
        kv_in[0] = kv_out[here]
        q_in[0, HEAD : 2 * HEAD, :] = q_out[here]

        def forward(n):
            return remote(kv_in.at[n], kv_in.at[PLANE + n], f_s.at[n], f_r.at[n], beside)

        def arrived(n):
            remote(kv_in.at[n], kv_in.at[n], kv_s.at[n], kv_r.at[n], beside).wait_recv()

        def asked(n):
            remote(
                q_in.at[n, HEAD : 2 * HEAD], q_in.at[n, HEAD : 2 * HEAD], q_s.at[n], q_r.at[n], beside
            ).wait_recv()

        for n in range(1, ROW):
            arrived(n)
            forward(n).start()
        for n in range(1, group):
            asked(n)
        for copy in loads:
            copy.start()

        ones = jnp.where(
            lax.broadcasted_iota(jnp.int32, (VROWS - HEAD, 128), 0) == 0, 1.0, 0.0
        ).astype(BF16)

        def scores(spot, c, h, upper):
            stage, g = spot
            keys = kv_in[pl.ds(stage * ROW + 2 * c, 2), 0:128, :].reshape(256, 128)
            at = 0 if upper else HEAD
            asking = jnp.concatenate(
                [q_in[g * group + 2 * h + k, at : at + 128, :] for k in range(2)], axis=1
            )
            return jnp.dot(keys, asking, preferred_element_type=F32)

        def values(spot, c):
            n = spot[0] * ROW + 2 * c
            pieces = []
            for at in (128, 128 + HEAD):
                for k in range(2):
                    pieces.append(
                        jnp.concatenate([kv_in[n + k, at : at + HEAD, :], ones], axis=0)
                    )
            return jnp.concatenate(pieces, axis=1)

        for g in range(2):
            high_s[g] = jnp.full((1, queries), -1e30, F32)
            total_s[g] = jnp.zeros((VROWS, queries), F32)

        def ahead(slot, spot, c, h):
            top = None
            span = slice(h * strip, (h + 1) * strip)
            for upper in range(2):
                piece = scores(spot, c, h, upper)
                score[slot, upper * 256 : (upper + 1) * 256, span] = piece
                piece = jnp.max(piece, axis=0, keepdims=True)
                top = piece if top is None else jnp.maximum(top, piece)
            return top

        def take(stage):
            for k in range(ROW):
                arrived(stage * ROW + k)
                forward(stage * ROW + k).start()

        def take_beside(stage):
            for k in range(ROW):
                forward(stage * ROW + k).wait_recv()

        def advance(spot, c, after, c_after, highest, total, top, finish=None):
            raised = jnp.maximum(highest, top)
            fade = jnp.exp2(highest - raised)
            values_now = values(spot, c)
            tops, totals = [], []
            for h in range(queries // strip):
                span = slice(h * strip, (h + 1) * strip)
                piece = total[:, span] * fade[:, span]
                best = None
                for upper in range(2):
                    rows = slice(upper * 256, (upper + 1) * 256)
                    if after is not None:
                        coming = scores(after, c_after, h, upper)
                    weights = jnp.exp2(score[c, rows, span] - raised[:, span]).astype(BF16)
                    if after is not None:
                        score[1 - c, rows, span] = coming
                        coming = jnp.max(coming, axis=0, keepdims=True)
                        best = coming if best is None else jnp.maximum(best, coming)
                    piece = piece + jnp.dot(
                        values_now[:, rows], weights, preferred_element_type=F32
                    )
                tops.append(best)
                totals.append(piece)
                if finish is not None:
                    finish(spot[1], h, piece)
            if after is not None:
                top = jnp.concatenate(tops, axis=1)
            return raised, jnp.concatenate(totals, axis=1), top

        def stage_at(it):
            return jnp.where(it == 1, ROW, jnp.where(it <= ROW, it - 1, it))

        def body(it, top):
            stage, coming_stage = stage_at(it), stage_at(it + 1)
            for g in range(2):
                highest, total = high_s[g], total_s[g]
                highest, total, top = advance((stage, g), 0, (stage, g), 1, highest, total, top)
                if g == 1:

                    @pl.when(it < ROW)
                    def _():
                        take(it)

                    @pl.when(it >= ROW)
                    def _():
                        take_beside(it - (ROW - 1))

                after = (stage, 1) if g == 0 else (coming_stage, 0)
                highest, total, top = advance((stage, g), 1, after, 0, highest, total, top)
                high_s[g] = highest
                total_s[g] = total
            return top

        def finish(g, h, piece):
            mixed = (piece[0:HEAD] / piece[HEAD : HEAD + 1]).astype(BF16)
            for k in range(2):
                n = g * group + 2 * h + k
                o_out[n] = mixed[:, k * tokens : (k + 1) * tokens]
                if n:
                    i, j = order[n][0], order[n][1]
                    source = lax.rem(y + ROW - i, ROW) * ROW + lax.rem(x + ROW - j, ROW)
                    remote(
                        o_out.at[n], att.at[here], o_s.at[n], o_r.at[n], half * PLANE + source
                    ).start()

        top = jnp.concatenate(
            [ahead(0, (0, 0), 0, h) for h in range(queries // strip)], axis=1
        )
        for g in range(2):
            highest, total, top = advance((0, g), 0, (0, g), 1, high_s[g], total_s[g], top)
            if g == 0:
                for n in range(group, PLANE):
                    asked(n)
            else:
                take_beside(0)
            after = (0, 1) if g == 0 else (ROW, 0)
            highest, total, top = advance((0, g), 1, after, 0, highest, total, top)
            high_s[g] = highest
            total_s[g] = total
        top = lax.fori_loop(1, stages - 1, body, top)
        last = stages - 1
        for g in range(2):
            highest, total, top = advance(
                (last, g), 0, (last, g), 1, high_s[g], total_s[g], top
            )
            after = (last, 1) if g == 0 else None
            highest, total, top = advance(
                (last, g), 1, after, 0, highest, total, top, finish
            )
        att[here] = o_out[0]

        def returned(n):
            head = order[n][2] * ROW + order[n][3]
            return remote(o_out.at[n], att.at[head], o_s.at[n], o_r.at[n], beside)

        loads[0].wait()
        summed = resv[...].astype(F32) + ob_ref[...]
        for g in range(ROW):
            for n in range(g * ROW, (g + 1) * ROW):
                if n:
                    returned(n).wait_recv()
            row = order[g * ROW][2]
            attended = att[pl.ds(row * ROW, ROW)].reshape(ROW * HEAD, tokens).T
            at = pl.multiple_of(row * ROW * HEAD, ROW * HEAD)
            summed = summed + jnp.dot(
                attended, wo[pl.ds(at, ROW * HEAD), :], preferred_element_type=F32
            )
        stream = summed.astype(BF16)
        rows = stream.astype(F32)
        normed_two = normalize(rows, g2_ref[...], s2_ref[...]).astype(BF16)
        loads[1].wait()
        loads[2].wait()

        def expand(c):
            span = slice(c * step, (c + 1) * step)
            return (
                jnp.dot(normed_two, w1v[:, span], preferred_element_type=F32) + b1_ref[:, span]
            )

        total = rows + b2_ref[...]
        coming = expand(0)
        for c in range(hidden_width // step):
            hidden = coming
            if c + 1 < hidden_width // step:
                coming = expand(c + 1)
            hidden = 0.5 * hidden * (1.0 + lax.erf(hidden * math.sqrt(0.5)))
            total = total + jnp.dot(
                hidden.astype(BF16), w2v[c * step : (c + 1) * step, :], preferred_element_type=F32
            )
        out_ref[...] = total.astype(BF16)
        for n in range(1, PLANE):
            returned(n).wait_send()
        for n in range(1, PLANE):
            kv_copy(n).wait_send()
            q_copy(n).wait_send()
        for n in range(PLANE):
            forward(n).wait_send()

    vmem = pl.BlockSpec(memory_space=pltpu.VMEM)
    anywhere = pl.BlockSpec(memory_space=pl.ANY)
    dma = pltpu.SemaphoreType.DMA
    return pl.pallas_call(
        kernel,
        in_specs=[anywhere] * 16,
        out_specs=vmem,
        out_shape=jax.ShapeDtypeStruct((tokens, width), BF16),
        scratch_shapes=[
            pltpu.VMEM(density.shape, F32),
            pltpu.VMEM(stem_weight.shape, BF16),
            pltpu.VMEM(stem_bias.shape, F32),
            pltpu.VMEM(gain1.shape, F32),
            pltpu.VMEM(shift1.shape, F32),
            pltpu.VMEM(qkv_bias.shape, F32),
            pltpu.VMEM(out_bias.shape, F32),
            pltpu.VMEM(gain2.shape, F32),
            pltpu.VMEM(shift2.shape, F32),
            pltpu.VMEM(b1.shape, F32),
            pltpu.VMEM(b2.shape, F32),
            pltpu.VMEM((1, 128), F32),
            pltpu.VMEM((count - 1, 1, 128), F32),
            pltpu.VMEM((2, side, side), F32),
            pltpu.VMEM((6 * pad, 128), F32),
            pltpu.VMEM((6, side, lanes), BF16),
            pltpu.VMEM((tokens, tokens), BF16),
            pltpu.VMEM((tokens, 6 * 128), BF16),
            pltpu.VMEM((6 * 128, width), BF16),
            pltpu.VMEM(w_qkv.shape, BF16),
            pltpu.VMEM(pos.shape, BF16),
            pltpu.VMEM(w_out.shape, BF16),
            pltpu.VMEM(w1.shape, BF16),
            pltpu.VMEM(w2.shape, BF16),
            pltpu.VMEM((tokens, width), BF16),
            pltpu.VMEM((HEADS, HEAD, tokens), BF16),
            pltpu.VMEM((HEADS, 256, 128), BF16),
            pltpu.VMEM((PLANE, 3 * HEAD, tokens), BF16),
            pltpu.VMEM((2 * PLANE, 256, 128), BF16),
            pltpu.VMEM((2, chunk, queries), F32),
            pltpu.VMEM((2, 1, queries), F32),
            pltpu.VMEM((2, VROWS, queries), F32),
            pltpu.VMEM((PLANE, HEAD, tokens), BF16),
            pltpu.VMEM((HEADS, HEAD, tokens), BF16),
            dma((count - 1,)), dma((count - 1,)), dma((2,)), dma((2,)),
            dma((PLANE,)), dma((PLANE,)), dma((PLANE,)), dma((PLANE,)),
            dma((PLANE,)), dma((PLANE,)), dma((PLANE,)), dma((PLANE,)), dma((16,)),
        ],
        compiler_params=pltpu.CompilerParams(
            vmem_limit_bytes=VMEM_LIMIT, collective_id=0, has_side_effects=True
        ),
        name="encoder",
    )(
        density, stem_weight, stem_bias, pos, gain1, shift1, w_qkv, qkv_bias,
        w_out, out_bias, gain2, shift2, w1, b1, w2, b2,
    )


def per_device(
    density, stem_weight, stem_bias, pos_embed, ln1_gain, ln1_bias, w_qkv, qkv_bias,
    w_out, out_bias, ln2_gain, ln2_bias, w_fc1, fc1_bias, w_fc2, fc2_bias,
):
    def flat(vector):
        return vector.reshape(1, -1)

    return encoder(
        density, stem_weight, flat(stem_bias), pos_embed, flat(ln1_gain), flat(ln1_bias),
        w_qkv, flat(qkv_bias), w_out, flat(out_bias), flat(ln2_gain), flat(ln2_bias),
        w_fc1, flat(fc1_bias), w_fc2, flat(fc2_bias),
        float(density.size * lax.axis_size("ctx")),
    )


def solution(mesh):
    in_specs = (P(("dp", "ctx"), None, None), P(), P(), P("ctx", None)) + (P(),) * 12
    return jax.shard_map(
        per_device, mesh=mesh, in_specs=in_specs, out_specs=P(("dp", "ctx"), None), check_vma=False
    )
```
